32 devices in a mesh: dp: 4 (over y, z), sp: 8 (over x, core).
Axes of the slice: x: 4, y: 2, z: 2, core: 2. Of those that a mesh axis runs over, the one named last changes fastest.
The devices are a block of a 4x4x8 slice.
Arguments:
- hidden: bfloat16 [4096, 2048], P(('dp', 'sp')), parts along dimension 0
- ln_gain: bfloat16 [2048], replicated
- w_q: bfloat16 [2048, 4096], replicated
- w_k: bfloat16 [2048, 512], replicated
- w_v: bfloat16 [2048, 512], replicated
- w_o: bfloat16 [4096, 2048], replicated
- q_gain: bfloat16 [128], replicated
- k_gain: bfloat16 [128], replicated
Outputs:
- output: bfloat16 [4096, 2048], P(('dp', 'sp')), parts along dimension 0
There are 4 independent parts. The reference program is written for one: setup_inputs(seed, part) draws one part's arguments, and reference() takes and returns one part's arrays. A program takes and returns all parts, laid end to end along the dimension named above; an argument that names none is the same for every part.
All inputs are finite; a program needn't handle non-finite values.
Results may differ from the reference program's by a relative error of at most 0.00713517.
Values are sent between devices in bfloat16 or wider.
A program may use at most 768 MiB of HBM per device.

```python
import math
import jax
import jax.numpy as jnp
from jax import lax

D = 2048
HEADS = 32
KV_HEADS = 4
HEAD = 128
SEQ = 1024
EPS = 1e-6
THETA = 1000000.0


def setup_inputs(seed: int = 0, part: int = 0) -> dict:
    keys = jax.random.split(jax.random.key(seed), 7)
    part_key = jax.random.fold_in(jax.random.key(seed + 1), part)
    gain_scale = math.log(SEQ / 8.0) ** 0.25
    hidden = jax.random.normal(part_key, (SEQ, D), jnp.float32)
    ln_gain = 1.0 + 0.3 * jax.random.normal(keys[0], (D,), jnp.float32)
    w_q = jax.random.normal(keys[1], (D, HEADS * HEAD), jnp.float32) * D ** -0.5
    w_k = jax.random.normal(keys[2], (D, KV_HEADS * HEAD), jnp.float32) * D ** -0.5
    w_v = jax.random.normal(keys[3], (D, KV_HEADS * HEAD), jnp.float32) * D ** -0.5
    w_o = jax.random.normal(keys[4], (HEADS * HEAD, D), jnp.float32) * (2.0 * (HEADS * HEAD) ** -0.5)
    q_gain = gain_scale * (1.0 + 0.2 * jax.random.normal(keys[5], (HEAD,), jnp.float32))
    k_gain = gain_scale * (1.0 + 0.2 * jax.random.normal(keys[6], (HEAD,), jnp.float32))
    return {
        'hidden': hidden.astype(jnp.bfloat16),
        'ln_gain': ln_gain.astype(jnp.bfloat16),
        'w_q': w_q.astype(jnp.bfloat16),
        'w_k': w_k.astype(jnp.bfloat16),
        'w_v': w_v.astype(jnp.bfloat16),
        'w_o': w_o.astype(jnp.bfloat16),
        'q_gain': q_gain.astype(jnp.bfloat16),
        'k_gain': k_gain.astype(jnp.bfloat16),
    }


def head_norm(values, gain):
    return values * lax.rsqrt(jnp.mean(values * values, axis=-1, keepdims=True) + EPS) * gain.astype(jnp.float32)


def rotate(values, positions):
    half = HEAD // 2
    inv_freq = jnp.power(THETA, -(jnp.arange(half, dtype=jnp.float32) * (2.0 / HEAD)))
    angles = positions.astype(jnp.float32)[:, None] * inv_freq[None, :]
    cos_pos = jnp.cos(angles)[:, None, :]
    sin_pos = jnp.sin(angles)[:, None, :]
    first_half = values[..., :half]
    second_half = values[..., half:]
    return jnp.concatenate([first_half * cos_pos - second_half * sin_pos, second_half * cos_pos + first_half * sin_pos], axis=-1)


def attend(q_all, k_all, v_all):
    limit = 2 ** 25 // (HEADS * SEQ)
    block_rows = min(SEQ, 2 ** max(3, min(9, limit.bit_length() - 1)))
    num_blocks = SEQ // block_rows
    group = HEADS // KV_HEADS
    q_blocks = q_all.reshape(num_blocks, block_rows, KV_HEADS, group, HEAD)
    key_pos = jnp.arange(SEQ)
    k_f32 = k_all.astype(jnp.float32)
    v_f32 = v_all.astype(jnp.float32)

    def one_block(block_args):
        q_block, block_idx = block_args
        scores = jnp.einsum('qkgd,skd->kgqs', q_block.astype(jnp.float32), k_f32) * (HEAD ** -0.5)
        q_pos = block_idx * block_rows + jnp.arange(block_rows)
        visible = q_pos[:, None] >= key_pos[None, :]
        scores = jnp.where(visible, scores, -jnp.inf)
        attn_prob = jax.nn.softmax(scores, axis=-1).astype(jnp.bfloat16)
        mixed = jnp.einsum('kgqs,skd->qkgd', attn_prob.astype(jnp.float32), v_f32)
        return mixed.astype(jnp.bfloat16)

    outputs = lax.map(one_block, (q_blocks, jnp.arange(num_blocks)))
    return outputs.reshape(SEQ, HEADS, HEAD)


def reference(hidden, ln_gain, w_q, w_k, w_v, w_o, q_gain, k_gain):
    hidden_f32 = hidden.astype(jnp.float32)
    normed = (hidden_f32 * lax.rsqrt(jnp.mean(hidden_f32 * hidden_f32, axis=-1, keepdims=True) + EPS) * ln_gain.astype(jnp.float32)).astype(jnp.bfloat16)
    positions = jnp.arange(SEQ)
    q_raw = jnp.dot(normed, w_q, preferred_element_type=jnp.float32).reshape(SEQ, HEADS, HEAD)
    k_raw = jnp.dot(normed, w_k, preferred_element_type=jnp.float32).reshape(SEQ, KV_HEADS, HEAD)
    v_all = jnp.dot(normed, w_v, preferred_element_type=jnp.float32).astype(jnp.bfloat16).reshape(SEQ, KV_HEADS, HEAD)
    q_all = rotate(head_norm(q_raw, q_gain), positions).astype(jnp.bfloat16)
    k_all = rotate(head_norm(k_raw, k_gain), positions).astype(jnp.bfloat16)
    mixed = attend(q_all, k_all, v_all)
    result = hidden_f32 + jnp.dot(mixed.reshape(SEQ, HEADS * HEAD), w_o, preferred_element_type=jnp.float32)
    return result.astype(jnp.bfloat16)
```

```python
import functools
import numpy as np
import jax
import jax.numpy as jnp
from jax import lax
from jax.experimental import pallas as pl
from jax.experimental.pallas import tpu as pltpu
from jax.sharding import PartitionSpec as P

EPS = 1e-6
THETA = 1000000.0
LOG2E = 1.4426950408889634
MESH = pl.DeviceIdType.MESH
CORES = 2
CHIPS = 4
BF16 = jnp.bfloat16
F32 = jnp.float32


def rope_tables(rows, head_dim):
    half = head_dim // 2
    inv_freq = np.power(np.float32(THETA), -(np.arange(half, dtype=np.float32) * np.float32(2.0 / head_dim)))
    angles = np.arange(rows, dtype=np.float32)[:, None] * inv_freq.astype(np.float32)[None, :]
    cos = np.cos(angles.astype(np.float64)).astype(np.float32)
    sin = np.sin(angles.astype(np.float64)).astype(np.float32)
    return np.concatenate([cos, cos], axis=1), np.concatenate([-sin, sin], axis=1)


def kernel(x_hbm, ln_hbm, wq_hbm, wk_hbm, wv_hbm, wo_hbm, qg_hbm, kg_hbm, cos_hbm, sin_hbm, out_hbm,
           x_v, ln_v, qg_v, kg_v, cos_v, sin_v, wkv_v, wq_v, wo_v, h_v, pk_v, kv_v, q_v, acc_v, m_v, l_v,
           o_v, os_v, y_v, out_v,
           ld_sem, wkv_sem, wq_sem, wo_sem, out_sem, h_sem, kvp_sem, kvu_sem, kvd_sem, rel_sem, kv_sem, o_sem):
    rows, feats = x_v.shape[1], x_v.shape[2]
    head = cos_v.shape[-1]
    pair = CORES * rows
    halves = wkv_v.shape[0]
    group = q_v.shape[0] // halves
    width = group * head
    scale = head ** -0.5 * LOG2E
    qcols = wq_v.shape[2]
    qparts = width // qcols
    ocols = 512

    dp = lax.axis_index("dp")
    sp = lax.axis_index("sp")
    c = lax.div(sp, CORES)
    s = lax.rem(sp, CORES)
    mate = c * CORES + (1 - s)
    up = lax.rem(c + 1, CHIPS)
    down = lax.rem(c + CHIPS - 1, CHIPS)
    first, last = c == 0, c == CHIPS - 1
    mine = c * CORES + s

    def dev(chip, core):
        return (dp, chip * CORES + core)

    loads = [
        pltpu.make_async_copy(x_hbm, x_v.at[0], ld_sem.at[0]),
        pltpu.make_async_copy(ln_hbm, ln_v, ld_sem.at[1]),
        pltpu.make_async_copy(qg_hbm, qg_v, ld_sem.at[2]),
        pltpu.make_async_copy(kg_hbm, kg_v, ld_sem.at[3]),
        pltpu.make_async_copy(cos_hbm.at[pl.ds(pl.multiple_of(c * pair, pair), pair)], cos_v, ld_sem.at[4]),
        pltpu.make_async_copy(sin_hbm.at[pl.ds(pl.multiple_of(c * pair, pair), pair)], sin_v, ld_sem.at[5]),
    ]
    kvw = CORES * head

    def wkv_load(j, which):
        src = (wk_hbm, wv_hbm)[which]
        return pltpu.make_async_copy(src.at[:, pl.ds(j * kvw, kvw)], wkv_v.at[j, :, pl.ds(which * kvw, kvw)], wkv_sem.at[j, which])

    def wq_load(i):
        j, part = divmod(i, qparts)
        col = (CORES * j + s) * width + part * qcols
        return pltpu.make_async_copy(wq_hbm.at[:, pl.ds(pl.multiple_of(col, qcols), qcols)], wq_v.at[i], wq_sem.at[i])

    def wo_load(i):
        return pltpu.make_async_copy(wo_hbm.at[pl.ds(i * width, width)], wo_v.at[i], wo_sem.at[i])

    n_wq = halves * qparts
    n_wo = CORES * halves
    loads[0].start()
    loads[1].start()
    for j in range(halves):
        wkv_load(j, 0).start()
        wkv_load(j, 1).start()
        if j == 0:
            for load in loads[2:]:
                load.start()
    for i in range(n_wq):
        wq_load(i).start()

    barrier = pltpu.get_barrier_semaphore()
    pl.semaphore_signal(barrier, inc=1, device_id=(dp, mate), device_id_type=MESH)
    for chip in (up, down):
        for core in range(CORES):
            pl.semaphore_signal(barrier, inc=1, device_id=dev(chip, core), device_id_type=MESH)

    def remote(src, dst, send, recv, to):
        return pltpu.make_async_remote_copy(src_ref=src, dst_ref=dst, send_sem=send, recv_sem=recv, device_id=to, device_id_type=MESH)

    h_copy = remote(h_v.at[s], h_v.at[s], h_sem.at[0], h_sem.at[1], (dp, mate))

    def to_mate(j):
        return remote(pk_v.at[j, 1 - s], kv_v.at[j, mine], kvp_sem.at[j], kv_sem.at[j, mine], (dp, mate))

    def to_up(j, core):
        return remote(pk_v.at[j, core], kv_v.at[j, mine], kvu_sem.at[j, core], kv_sem.at[j, mine], dev(up, core))

    def to_down(j, core):
        return remote(pk_v.at[j, core], kv_v.at[j, mine], kvd_sem.at[j, core], kv_sem.at[j, mine], dev(down, core))

    def relay(j, block, slot, chip):
        return remote(kv_v.at[j, block], kv_v.at[j, block], rel_sem.at[j, slot], kv_sem.at[j, block], dev(chip, s))

    def kv_wait(j, block):
        remote(kv_v.at[j, block], kv_v.at[j, block], kvp_sem.at[0], kv_sem.at[j, block], (dp, mate)).wait_recv()

    def o_copy(j):
        return remote(os_v.at[j], o_v.at[CORES * j + s], o_sem.at[0, j], o_sem.at[1, CORES * j + s], (dp, mate))

    sends_down = jnp.logical_or(first, jnp.logical_and(c == 1, s == 1))

    loads[0].wait()
    loads[1].wait()
    gain = ln_v[...].astype(F32).reshape(1, feats)
    step = 32

    def norm_rows(r, _):
        x = x_v[0, pl.ds(pl.multiple_of(r * step, step), step), :].astype(F32)
        inv = lax.rsqrt(jnp.mean(x * x, axis=-1, keepdims=True) + EPS)
        h_v[s, pl.ds(pl.multiple_of(r * step, step), step), :] = (x * inv * gain).astype(BF16)
        return 0

    lax.fori_loop(0, rows // step, norm_rows, 0)
    pl.semaphore_wait(barrier, 1 + 2 * CORES)
    h_copy.start()
    for load in loads[2:]:
        load.wait()
    q_gain = qg_v[...].astype(F32).reshape(1, head)
    k_gain = kg_v[...].astype(F32).reshape(1, head)

    def norm_rope(t, g, cos, sin):
        t = t * lax.rsqrt(jnp.mean(t * t, axis=-1, keepdims=True) + EPS) * g
        return (t * cos + pltpu.roll(t, head // 2, 1) * sin).astype(BF16)

    for j in range(halves):
        wkv_load(j, 0).wait()
        wkv_load(j, 1).wait()
        raw = jnp.dot(h_v[s], wkv_v[j], preferred_element_type=F32)
        own = pl.ds(pl.multiple_of(s * rows, rows), rows)
        cos, sin = cos_v[own, :], sin_v[own, :]
        for core in range(CORES):
            pk_v[j, core, 0] = norm_rope(raw[:, core * head:(core + 1) * head], k_gain, cos, sin)
            pk_v[j, core, 1] = raw[:, kvw + core * head:kvw + (core + 1) * head].astype(BF16)
        for core in range(CORES):
            @pl.when(jnp.logical_not(last))
            def _():
                to_up(j, core).start()

            @pl.when(sends_down)
            def _():
                to_down(j, core).start()
        to_mate(j).start()
        kv_v[j, mine] = pk_v[j, s]

    h_copy.wait_recv()

    def project_q(i, _):
        pltpu.make_async_copy(wq_hbm.at[:, pl.ds(0, qcols)], wq_v.at[i], wq_sem.at[i]).wait()
        raw = jnp.dot(h_v[...].reshape(pair, feats), wq_v[i], preferred_element_type=F32)
        for g in range(qcols // head):
            q_v[i * (qcols // head) + g] = norm_rope(raw[:, g * head:(g + 1) * head], q_gain, cos_v[...], sin_v[...])
        return 0

    for i in range(n_wo):
        wo_load(i).start()
    lax.fori_loop(0, n_wq, project_q, 0)

    @pl.when(first)
    def _():
        for j in range(halves):
            kv_wait(j, 2 * CORES - 1)
            relay(j, 2 * CORES - 1, 0, down).start()

    def attend(j, block, diagonal):
        keys = kv_v[j, pl.ds(block * CORES, CORES), 0].reshape(pair, head)
        vals = kv_v[j, pl.ds(block * CORES, CORES), 1].reshape(pair, head)
        if diagonal:
            row = lax.broadcasted_iota(jnp.int32, (pair, pair), 0)
            col = lax.broadcasted_iota(jnp.int32, (pair, pair), 1)
            seen = row >= col
        for g in range(group):
            i = j * group + g
            sc = lax.dot_general(q_v[i], keys, (((1,), (1,)), ((), ())), preferred_element_type=F32)
            if diagonal:
                sc = jnp.where(seen, sc, -jnp.inf)
            top = jnp.max(sc, axis=-1, keepdims=True) * scale
            if diagonal:
                new = jnp.broadcast_to(top, (pair, head))
            else:
                old = m_v[i]
                new = jnp.maximum(old, top)
            m_v[i] = new
            probs = [jnp.exp2(sc[:, k * head:(k + 1) * head] * scale - new) for k in range(pair // head)]
            total = sum(probs[1:], probs[0])
            mixed = jnp.dot(jnp.concatenate(probs, axis=1).astype(BF16), vals, preferred_element_type=F32)
            if diagonal:
                l_v[i] = total
                acc_v[i] = mixed
            else:
                fade = jnp.exp2(old - new)
                l_v[i] = l_v[i] * fade + total
                acc_v[i] = acc_v[i] * fade + mixed

    def project_out(i, final):
        for n in range(feats // ocols):
            cols = slice(n * ocols, (n + 1) * ocols)
            part = jnp.dot(o_v[i], wo_v[i, :, cols], preferred_element_type=F32)
            y_v[:, cols] += part

    y_v[...] = x_v[0].astype(F32)

    def one_step(idx, _):
        t = lax.div(idx, halves)
        j = lax.rem(idx, halves)

        @pl.when(t == 0)
        def _():
            kv_wait(j, mate)
            attend(j, c, True)

        @pl.when(t > 0)
        def _():
            block = c - t + lax.div(c, CHIPS - 1) * lax.div(t, 2) * (2 * lax.rem(t, 2) - 1)

            @pl.when(jnp.logical_or(jnp.logical_not(last), t != 2))
            def _():
                for core in range(CORES):
                    kv_wait(j, block * CORES + core)

            @pl.when(jnp.logical_and(c == 2, t == 1))
            def _():
                relay(j, CORES, 0, up).start()

            @pl.when(jnp.logical_and(last, t == 1))
            def _():
                for core in range(CORES):
                    kv_wait(j, core)
                    relay(j, core, core, down).start()

            attend(j, block, False)

        @pl.when(t == c)
        def _():
            for g in range(group):
                i = j * group + g
                inv = 1.0 / jnp.sum(l_v[i], axis=-1, keepdims=True)
                o = (acc_v[i] * inv).astype(BF16)
                acc_v[i] = acc_v[i] * inv
            for g in range(group):
                i = j * group + g
                theirs = pl.ds(pl.multiple_of((1 - s) * rows, rows), rows)
                ours = pl.ds(pl.multiple_of(s * rows, rows), rows)
                os_v[j, :, g * head:(g + 1) * head] = acc_v[i, theirs, :].astype(BF16)
                o_v[CORES * j + s, :, g * head:(g + 1) * head] = acc_v[i, ours, :].astype(BF16)
            o_copy(j).start()
            i = CORES * j + s
            pltpu.make_async_copy(wo_hbm.at[pl.ds(0, width)], wo_v.at[i], wo_sem.at[i]).wait()
            project_out(i, False)

        return 0

    lax.fori_loop(0, halves * (c + 1), one_step, 0)

    def theirs_out(j, _):
        i = CORES * j + 1 - s
        remote(os_v.at[j], o_v.at[i], o_sem.at[0, j], o_sem.at[1, i], (dp, mate)).wait_recv()
        pltpu.make_async_copy(wo_hbm.at[pl.ds(0, width)], wo_v.at[i], wo_sem.at[i]).wait()
        project_out(i, False)
        return 0

    lax.fori_loop(0, halves, theirs_out, 0)
    out_v[...] = y_v[...].astype(BF16)
    out = pltpu.make_async_copy(out_v, out_hbm, out_sem)
    out.start()

    h_copy.wait_send()
    for j in range(halves):
        to_mate(j).wait_send()
        o_copy(j).wait_send()
        for core in range(CORES):
            @pl.when(jnp.logical_not(last))
            def _():
                to_up(j, core).wait_send()

            @pl.when(sends_down)
            def _():
                to_down(j, core).wait_send()

            @pl.when(last)
            def _():
                relay(j, core, core, down).wait_send()

        @pl.when(first)
        def _():
            relay(j, 2 * CORES - 1, 0, down).wait_send()

        @pl.when(c == 2)
        def _():
            relay(j, CORES, 0, up).wait_send()
    out.wait()


def solution(mesh):
    group_size = mesh.shape['sp']
    assert group_size == CORES * CHIPS

    def device_step(hidden, ln_gain, w_q, w_k, w_v, w_o, q_gain, k_gain):
        rows, feats = hidden.shape
        head = q_gain.shape[0]
        kv_heads = w_k.shape[1] // head
        q_heads = w_q.shape[1] // head
        halves = kv_heads // CORES
        group = q_heads // kv_heads
        width = group * head
        pair = CORES * rows
        qcols = 512
        n_wq = halves * width // qcols
        cos, sin = rope_tables(group_size * rows, head)
        dma = pltpu.SemaphoreType.DMA
        any_spec = pl.BlockSpec(memory_space=pl.ANY)
        scratch = [
            pltpu.VMEM((1, rows, feats), BF16),
            pltpu.VMEM((1, feats), BF16),
            pltpu.VMEM((1, head), BF16),
            pltpu.VMEM((1, head), BF16),
            pltpu.VMEM((pair, head), F32),
            pltpu.VMEM((pair, head), F32),
            pltpu.VMEM((halves, feats, 2 * CORES * head), BF16),
            pltpu.VMEM((n_wq, feats, qcols), BF16),
            pltpu.VMEM((kv_heads, width, feats), BF16),
            pltpu.VMEM((CORES, rows, feats), BF16),
            pltpu.VMEM((halves, CORES, 2, rows, head), BF16),
            pltpu.VMEM((halves, group_size, 2, rows, head), BF16),
            pltpu.VMEM((halves * group, pair, head), BF16),
            pltpu.VMEM((halves * group, pair, head), F32),
            pltpu.VMEM((halves * group, pair, head), F32),
            pltpu.VMEM((halves * group, pair, head), F32),
            pltpu.VMEM((kv_heads, rows, width), BF16),
            pltpu.VMEM((halves, rows, width), BF16),
            pltpu.VMEM((rows, feats), F32),
            pltpu.VMEM((rows, feats), BF16),
            dma((6,)), dma((halves, 2)), dma((n_wq,)), dma((kv_heads,)), dma, dma((2,)),
            dma((halves,)), dma((halves, CORES)), dma((halves, CORES)), dma((halves, CORES)),
            dma((halves, group_size)), dma((2, kv_heads)),
        ]
        return pl.pallas_call(
            kernel,
            out_shape=jax.ShapeDtypeStruct((rows, feats), BF16),
            in_specs=[any_spec] * 10,
            out_specs=any_spec,
            scratch_shapes=scratch,
            compiler_params=pltpu.CompilerParams(
                collective_id=0, has_side_effects=True, vmem_limit_bytes=60 * 2 ** 20
            ),
            name="attention_block",
        )(hidden, ln_gain.reshape(1, -1), w_q, w_k, w_v, w_o, q_gain.reshape(1, -1), k_gain.reshape(1, -1),
          jnp.asarray(cos), jnp.asarray(sin))

    row_spec = P(('dp', 'sp'), None)
    return jax.shard_map(device_step, mesh=mesh, in_specs=(row_spec, P(), P(), P(), P(), P(), P(), P()), out_specs=row_spec, check_vma=False)
```

```python
import functools
import numpy as np
import jax
import jax.numpy as jnp
from jax import lax
from jax.experimental import pallas as pl
from jax.experimental.pallas import tpu as pltpu
from jax.sharding import PartitionSpec as P

EPS = 1e-6
THETA = 1000000.0
LOG2E = 1.4426950408889634
MESH = pl.DeviceIdType.MESH
CORES = 2
CHIPS = 4
BF16 = jnp.bfloat16
F32 = jnp.float32


def rope_tables(rows, head_dim):
    half = head_dim // 2
    inv_freq = np.power(np.float32(THETA), -(np.arange(half, dtype=np.float32) * np.float32(2.0 / head_dim)))
    angles = np.arange(rows, dtype=np.float32)[:, None] * inv_freq.astype(np.float32)[None, :]
    cos = np.cos(angles.astype(np.float64)).astype(np.float32)
    sin = np.sin(angles.astype(np.float64)).astype(np.float32)
    return np.concatenate([cos, cos], axis=1), np.concatenate([-sin, sin], axis=1)


def kernel(x_hbm, ln_hbm, wq_hbm, wk_hbm, wv_hbm, wo_hbm, qg_hbm, kg_hbm, rope_hbm, ropet_hbm, y_v,
           x_v, ln_v, qg_v, kg_v, rope_v, ropet_v, wkv_v, wq_v, wo_v, h_v, pk_v, kv_v, raw_v, q_v, s_v, acc_v, m_v, l_v,
           oo_v, or_v,
           ld_sem, wkv_sem, wq_sem, wo_sem, h_sem, kvp_sem, kvu_sem, kvd_sem, rel_sem, kv_sem, o_sem):
    rows, feats = x_v.shape[1], x_v.shape[2]
    head = rope_v.shape[-1]
    pair = CORES * rows
    halves = wkv_v.shape[0]
    group = q_v.shape[0] // halves
    width = group * head
    scale = head ** -0.5 * LOG2E
    qcols = wq_v.shape[2]
    qparts = width // qcols
    ocols = 512

    dp = lax.axis_index("dp")
    sp = lax.axis_index("sp")
    c = lax.div(sp, CORES)
    s = lax.rem(sp, CORES)
    mate = c * CORES + (1 - s)
    up = lax.rem(c + 1, CHIPS)
    down = lax.rem(c + CHIPS - 1, CHIPS)
    first, last = c == 0, c == CHIPS - 1
    mine = c * CORES + s

    def dev(chip, core):
        return (dp, chip * CORES + core)

    loads = [
        pltpu.make_async_copy(x_hbm, x_v.at[0], ld_sem.at[0]),
        pltpu.make_async_copy(ln_hbm, ln_v, ld_sem.at[1]),
        pltpu.make_async_copy(qg_hbm, qg_v, ld_sem.at[2]),
        pltpu.make_async_copy(kg_hbm, kg_v, ld_sem.at[3]),
        pltpu.make_async_copy(rope_hbm.at[c * CORES + s], rope_v, ld_sem.at[4]),
        pltpu.make_async_copy(ropet_hbm.at[c], ropet_v, ld_sem.at[5]),
    ]
    kvw = CORES * head

    def wkv_load(j, which):
        src = (wk_hbm, wv_hbm)[which]
        return pltpu.make_async_copy(src.at[:, pl.ds(j * kvw, kvw)], wkv_v.at[j, :, pl.ds(which * kvw, kvw)], wkv_sem.at[j, which])

    def wq_load(i):
        j, part = divmod(i, qparts)
        col = (CORES * j + s) * width + part * qcols
        return pltpu.make_async_copy(wq_hbm.at[:, pl.ds(pl.multiple_of(col, qcols), qcols)], wq_v.at[i], wq_sem.at[i])

    def wo_load(i):
        return pltpu.make_async_copy(wo_hbm.at[pl.ds(i * width, width)], wo_v.at[i], wo_sem.at[i])

    n_wq = halves * qparts
    n_wo = CORES * halves
    stages = [wkv_load(j, which) for j in range(halves) for which in range(2)]
    for load in loads[:5] + stages + loads[5:]:
        load.start()

    barrier = pltpu.get_barrier_semaphore()
    pl.semaphore_signal(barrier, inc=1, device_id=(dp, mate), device_id_type=MESH)
    for chip in (up, down):
        for core in range(CORES):
            pl.semaphore_signal(barrier, inc=1, device_id=dev(chip, core), device_id_type=MESH)

    def remote(src, dst, send, recv, to):
        return pltpu.make_async_remote_copy(src_ref=src, dst_ref=dst, send_sem=send, recv_sem=recv, device_id=to, device_id_type=MESH)

    h_copy = remote(h_v.at[s], h_v.at[s], h_sem.at[0], h_sem.at[1], (dp, mate))

    def to_mate(j):
        return remote(pk_v.at[j, 1 - s], kv_v.at[j, mine], kvp_sem.at[j], kv_sem.at[j, mine], (dp, mate))

    def to_up(j, core):
        return remote(pk_v.at[j, core], kv_v.at[j, mine], kvu_sem.at[j, core], kv_sem.at[j, mine], dev(up, core))

    def to_down(j, core):
        return remote(pk_v.at[j, core], kv_v.at[j, mine], kvd_sem.at[j, core], kv_sem.at[j, mine], dev(down, core))

    def relay(j, block, slot, chip):
        return remote(kv_v.at[j, block], kv_v.at[j, block], rel_sem.at[j, slot], kv_sem.at[j, block], dev(chip, s))

    def kv_wait(j, block):
        remote(kv_v.at[j, block], kv_v.at[j, block], kvp_sem.at[0], kv_sem.at[j, block], (dp, mate)).wait_recv()

    def o_copy(j):
        return remote(oo_v.at[j, 1 - s], or_v.at[j], o_sem.at[0, j], o_sem.at[1, j], (dp, mate))

    sends_down = jnp.logical_or(first, jnp.logical_and(c == 1, s == 1))

    loads[0].wait()
    loads[1].wait()
    gain = jnp.concatenate([ln_v[k:k + 1, :] for k in range(feats // head)], axis=1).astype(F32)
    step = 64

    def norm_rows(r, _):
        x = x_v[0, pl.ds(pl.multiple_of(r * step, step), step), :].astype(F32)
        inv = lax.rsqrt(jnp.mean(x * x, axis=-1, keepdims=True) + EPS)
        h_v[s, pl.ds(pl.multiple_of(r * step, step), step), :] = (x * inv * gain).astype(BF16)
        return 0

    lax.fori_loop(0, rows // step, norm_rows, 0)
    pl.semaphore_wait(barrier, 1 + 2 * CORES)
    h_copy.start()
    for load in loads[2:5]:
        load.wait()
    k_gain = kg_v[...].astype(F32).reshape(1, head)

    def norm_rope(t, g, cos, sin):
        t = t * lax.rsqrt(jnp.mean(t * t, axis=-1, keepdims=True) + EPS) * g
        return (t * cos + pltpu.roll(t, head // 2, 1) * sin).astype(BF16)

    def finish_kv(j):
        for core in range(CORES):
            pk_v[j, core, 0] = norm_rope(raw_v[j, :rows, core * head:(core + 1) * head], k_gain, rope_v[0], rope_v[1])
            pk_v[j, core, 1] = raw_v[j, :rows, kvw + core * head:kvw + (core + 1) * head].T.astype(BF16)

    def send_kv(j):
        for core in range(CORES):
            @pl.when(jnp.logical_not(last))
            def _():
                to_up(j, core).start()

            @pl.when(sends_down)
            def _():
                to_down(j, core).start()
        to_mate(j).start()
        kv_v[j, mine] = pk_v[j, s]

    for j in range(halves):
        wkv_load(j, 0).wait()
        wkv_load(j, 1).wait()
        for i in range(qparts):
            wq_load(qparts * j + i).start()
        raw_v[j, :rows] = jnp.dot(h_v[s], wkv_v[j], preferred_element_type=F32)
        if j:
            finish_kv(j - 1)
        if j:
            send_kv(j - 1)
    finish_kv(halves - 1)
    send_kv(halves - 1)

    h_copy.wait_recv()

    loads[5].wait()
    q_gain = jnp.broadcast_to(qg_v[...].astype(F32), (head, head)).T
    q_gain = jnp.concatenate([q_gain] * CORES, axis=1)

    def turn(t):
        return jnp.concatenate([t[head // 2:], t[:head // 2]], axis=0)

    ropet_v[0] = ropet_v[0] * q_gain
    ropet_v[1] = ropet_v[1] * turn(q_gain)

    def finish_q(i):
        for g in range(qcols // head):
            t = raw_v[i % 2, :, g * head:(g + 1) * head].T
            t = t * lax.rsqrt(jnp.mean(t * t, axis=0, keepdims=True) + EPS)
            q_v[i * (qcols // head) + g] = (t * ropet_v[0] + turn(t) * ropet_v[1]).astype(BF16)

    for i in range(n_wq):
        wq_load(i).wait()
        wo_load(i).start()
        raw_v[i % 2] = jnp.dot(h_v[...].reshape(pair, feats), wq_v[i], preferred_element_type=F32)
        if i:
            finish_q(i - 1)
    finish_q(n_wq - 1)

    @pl.when(first)
    def _():
        for j in range(halves):
            kv_wait(j, 2 * CORES - 1)
            relay(j, 2 * CORES - 1, 0, down).start()

    def relay_first(j):
        for core in range(CORES):
            kv_wait(j, core)
            relay(j, core, core, down).start()

    @pl.when(last)
    def _():
        relay_first(0)

    def attend(j, block, diagonal):
        keys = kv_v[j, pl.ds(block * CORES, CORES), 0].reshape(pair, head)
        vals = jnp.concatenate([kv_v[j, block * CORES + core, 1] for core in range(CORES)], axis=1)
        if diagonal:
            key = lax.broadcasted_iota(jnp.int32, (pair, pair), 0)
            row = lax.broadcasted_iota(jnp.int32, (pair, pair), 1)
            seen = key <= row

        def score(g):
            i = j * group + g
            sc = jnp.dot(keys, q_v[i], preferred_element_type=F32)
            if diagonal:
                sc = jnp.where(seen, sc, -jnp.inf)
            s_v[i] = sc
            return jnp.max(sc, axis=0, keepdims=True) * scale

        def mix(g, new):
            i = j * group + g
            if not diagonal:
                old = m_v[i]
                new = jnp.maximum(old, new)
            m_v[i] = new
            probs = jnp.exp2(s_v[i] * scale - new)
            total = jnp.sum(probs, axis=0, keepdims=True)
            mixed = jnp.dot(vals, probs.astype(BF16), preferred_element_type=F32)
            if diagonal:
                l_v[i] = total
                acc_v[i] = mixed
            else:
                fade = jnp.exp2(old - new)
                l_v[i] = l_v[i] * fade + total
                acc_v[i] = acc_v[i] * fade + mixed

        tops = [score(g) for g in range(group)]
        for g in range(group):
            mix(g, tops[g])

    def project_out(o_ref, i):
        for n in range(feats // ocols):
            cols = slice(n * ocols, (n + 1) * ocols)
            y_v[:, cols] += jnp.dot(o_ref[...], wo_v[i, :, cols], preferred_element_type=F32)

    y_v[...] = jnp.zeros_like(y_v)

    def one_step(idx, _):
        swap = lax.div(c, CHIPS - 1) * lax.rem(lax.div(idx + 2, 4), 2)
        t = (1 - swap) * lax.div(idx, 2) + swap * (1 + lax.rem(idx, 2))
        j = (1 - swap) * lax.rem(idx, 2) + swap * (lax.div(idx, 2) - 1)

        @pl.when(t == 0)
        def _():
            kv_wait(j, mate)
            attend(j, c, True)

        @pl.when(t > 0)
        def _():
            block = c - t + lax.div(c, CHIPS - 1) * lax.div(t, 2) * (2 * lax.rem(t, 2) - 1)

            @pl.when(jnp.logical_or(jnp.logical_not(last), t != 2))
            def _():
                for core in range(CORES):
                    kv_wait(j, block * CORES + core)

            @pl.when(jnp.logical_and(c == 2, t == 1))
            def _():
                relay(j, CORES, 0, up).start()

            @pl.when(jnp.logical_and(last, idx == halves + 1))
            def _():
                relay_first(1)

            attend(j, block, False)

        @pl.when(t == c)
        def _():
            for g in range(group):
                i = j * group + g
                o = acc_v[i] * (1.0 / l_v[i])
                for core in range(CORES):
                    oo_v[j, core, :, g * head:(g + 1) * head] = o[:, core * rows:(core + 1) * rows].T.astype(BF16)
            o_copy(j).start()
            i = CORES * j + s
            pltpu.make_async_copy(wo_hbm.at[pl.ds(0, width)], wo_v.at[i], wo_sem.at[i]).wait()
            project_out(oo_v.at[j, s], i)

        return 0

    lax.fori_loop(0, halves * (c + 1), one_step, 0)

    def theirs_out(j, _):
        i = CORES * j + 1 - s
        o_copy(j).wait_recv()
        pltpu.make_async_copy(wo_hbm.at[pl.ds(0, width)], wo_v.at[i], wo_sem.at[i]).wait()
        project_out(or_v.at[j], i)
        return 0

    lax.fori_loop(0, halves, theirs_out, 0)

    h_copy.wait_send()
    for j in range(halves):
        to_mate(j).wait_send()
        o_copy(j).wait_send()
        for core in range(CORES):
            @pl.when(jnp.logical_not(last))
            def _():
                to_up(j, core).wait_send()

            @pl.when(sends_down)
            def _():
                to_down(j, core).wait_send()

            @pl.when(last)
            def _():
                relay(j, core, core, down).wait_send()

        @pl.when(first)
        def _():
            relay(j, 2 * CORES - 1, 0, down).wait_send()

        @pl.when(c == 2)
        def _():
            relay(j, CORES, 0, up).wait_send()


def solution(mesh):
    group_size = mesh.shape['sp']
    assert group_size == CORES * CHIPS

    def device_step(hidden, ln_gain, w_q, w_k, w_v, w_o, q_gain, k_gain):
        rows, feats = hidden.shape
        head = q_gain.shape[0]
        kv_heads = w_k.shape[1] // head
        q_heads = w_q.shape[1] // head
        halves = kv_heads // CORES
        group = q_heads // kv_heads
        width = group * head
        pair = CORES * rows
        qcols = 512
        n_wq = halves * width // qcols
        tables = np.stack(rope_tables(group_size * rows, head))
        by_device = tables.reshape(2, group_size, rows, head).transpose(1, 0, 2, 3)
        by_chip = tables.reshape(2, CHIPS, pair, head).transpose(1, 0, 3, 2)
        dma = pltpu.SemaphoreType.DMA
        any_spec = pl.BlockSpec(memory_space=pl.ANY)
        scratch = [
            pltpu.VMEM((1, rows, feats), BF16),
            pltpu.VMEM((feats // head, head), BF16),
            pltpu.VMEM((1, head), BF16),
            pltpu.VMEM((1, head), BF16),
            pltpu.VMEM((2, rows, head), F32),
            pltpu.VMEM((2, head, pair), F32),
            pltpu.VMEM((halves, feats, 2 * CORES * head), BF16),
            pltpu.VMEM((n_wq, feats, qcols), BF16),
            pltpu.VMEM((kv_heads, width, feats), BF16),
            pltpu.VMEM((CORES, rows, feats), BF16),
            pltpu.VMEM((halves, CORES, 2, rows, head), BF16),
            pltpu.VMEM((halves, group_size, 2, rows, head), BF16),
            pltpu.VMEM((2, pair, qcols), F32),
            pltpu.VMEM((halves * group, head, pair), BF16),
            pltpu.VMEM((halves * group, pair, pair), F32),
            pltpu.VMEM((halves * group, head, pair), F32),
            pltpu.VMEM((halves * group, 1, pair), F32),
            pltpu.VMEM((halves * group, 1, pair), F32),
            pltpu.VMEM((halves, CORES, rows, width), BF16),
            pltpu.VMEM((halves, rows, width), BF16),
            dma((6,)), dma((halves, 2)), dma((n_wq,)), dma((kv_heads,)), dma((2,)),
            dma((halves,)), dma((halves, CORES)), dma((halves, CORES)), dma((halves, CORES)),
            dma((halves, group_size)), dma((2, halves)),
        ]
        mixed = pl.pallas_call(
            kernel,
            out_shape=pltpu.VMEM((rows, feats), F32),
            in_specs=[any_spec] * 10,
            out_specs=pl.BlockSpec(memory_space=pltpu.VMEM),
            scratch_shapes=scratch,
            compiler_params=pltpu.CompilerParams(
                collective_id=0, has_side_effects=True, vmem_limit_bytes=56 * 2 ** 20
            ),
            name="attention_block",
        )(hidden, ln_gain.reshape(-1, head), w_q, w_k, w_v, w_o, q_gain.reshape(1, -1), k_gain.reshape(1, -1),
          jnp.asarray(by_device), jnp.asarray(by_chip))
        return (hidden.astype(F32) + mixed).astype(BF16)

    row_spec = P(('dp', 'sp'), None)
    return jax.shard_map(device_step, mesh=mesh, in_specs=(row_spec, P(), P(), P(), P(), P(), P(), P()), out_specs=row_spec, check_vma=False)
```

```python
import functools
import numpy as np
import jax
import jax.numpy as jnp
from jax import lax
from jax.experimental import pallas as pl
from jax.experimental.pallas import tpu as pltpu
from jax.sharding import PartitionSpec as P

EPS = 1e-6
THETA = 1000000.0
LOG2E = 1.4426950408889634
MESH = pl.DeviceIdType.MESH
CORES = 2
CHIPS = 4
BF16 = jnp.bfloat16
F32 = jnp.float32


def rope_tables(rows, head_dim):
    half = head_dim // 2
    inv_freq = np.power(np.float32(THETA), -(np.arange(half, dtype=np.float32) * np.float32(2.0 / head_dim)))
    angles = np.arange(rows, dtype=np.float32)[:, None] * inv_freq.astype(np.float32)[None, :]
    cos = np.cos(angles.astype(np.float64)).astype(np.float32)
    sin = np.sin(angles.astype(np.float64)).astype(np.float32)
    return np.concatenate([cos, cos], axis=1), np.concatenate([-sin, sin], axis=1)


def kernel(x_hbm, ln_hbm, wq_hbm, wk_hbm, wv_hbm, wo_hbm, qg_hbm, kg_hbm, rope_hbm, ropet_hbm, y_v,
           x_v, ln_v, qg_v, kg_v, rope_v, ropet_v, wkv_v, wq_v, wo_v, h_v, pk_v, kv_v, raw_v, q_v, s_v, acc_v, m_v, l_v,
           oo_v, or_v,
           ld_sem, wkv_sem, wq_sem, wo_sem, h_sem, kvp_sem, kvu_sem, kvd_sem, rel_sem, kv_sem, o_sem):
    rows, feats = x_v.shape[1], x_v.shape[2]
    head = rope_v.shape[-1]
    pair = CORES * rows
    halves = wkv_v.shape[0]
    group = q_v.shape[0] // halves
    width = group * head
    scale = head ** -0.5 * LOG2E
    qcols = wq_v.shape[2]
    qparts = width // qcols
    ocols = 512

    dp = lax.axis_index("dp")
    sp = lax.axis_index("sp")
    c = lax.div(sp, CORES)
    s = lax.rem(sp, CORES)
    mate = c * CORES + (1 - s)
    up = lax.rem(c + 1, CHIPS)
    down = lax.rem(c + CHIPS - 1, CHIPS)
    first, last = c == 0, c == CHIPS - 1
    mine = c * CORES + s

    def dev(chip, core):
        return (dp, chip * CORES + core)

    loads = [
        pltpu.make_async_copy(x_hbm, x_v.at[0], ld_sem.at[0]),
        pltpu.make_async_copy(ln_hbm, ln_v, ld_sem.at[1]),
        pltpu.make_async_copy(qg_hbm, qg_v, ld_sem.at[2]),
        pltpu.make_async_copy(kg_hbm, kg_v, ld_sem.at[3]),
        pltpu.make_async_copy(rope_hbm.at[c * CORES + s], rope_v, ld_sem.at[4]),
        pltpu.make_async_copy(ropet_hbm.at[c], ropet_v, ld_sem.at[5]),
    ]
    kvw = CORES * head

    def wkv_load(j, which):
        src = (wk_hbm, wv_hbm)[which]
        return pltpu.make_async_copy(src.at[:, pl.ds(j * kvw, kvw)], wkv_v.at[j, :, pl.ds(which * kvw, kvw)], wkv_sem.at[j, which])

    def wq_load(i):
        j, part = divmod(i, qparts)
        col = (CORES * j + s) * width + part * qcols
        return pltpu.make_async_copy(wq_hbm.at[:, pl.ds(pl.multiple_of(col, qcols), qcols)], wq_v.at[i], wq_sem.at[i])

    def wo_load(i):
        return pltpu.make_async_copy(wo_hbm.at[pl.ds(i * width, width)], wo_v.at[i], wo_sem.at[i])

    n_wq = halves * qparts
    n_wo = CORES * halves
    stages = [wkv_load(j, which) for j in range(halves) for which in range(2)]
    for load in loads[:5] + stages:
        load.start()

    barrier = pltpu.get_barrier_semaphore()
    pl.semaphore_signal(barrier, inc=1, device_id=(dp, mate), device_id_type=MESH)
    for chip in (up, down):
        for core in range(CORES):
            pl.semaphore_signal(barrier, inc=1, device_id=dev(chip, core), device_id_type=MESH)

    def remote(src, dst, send, recv, to):
        return pltpu.make_async_remote_copy(src_ref=src, dst_ref=dst, send_sem=send, recv_sem=recv, device_id=to, device_id_type=MESH)

    h_copy = remote(h_v.at[s], h_v.at[s], h_sem.at[0], h_sem.at[1], (dp, mate))

    def to_mate(j):
        return remote(pk_v.at[j, 1 - s], kv_v.at[j, mine], kvp_sem.at[j], kv_sem.at[j, mine], (dp, mate))

    def to_up(j, core):
        return remote(pk_v.at[j, core], kv_v.at[j, mine], kvu_sem.at[j, core], kv_sem.at[j, mine], dev(up, core))

    def to_down(j, core):
        return remote(pk_v.at[j, core], kv_v.at[j, mine], kvd_sem.at[j, core], kv_sem.at[j, mine], dev(down, core))

    def relay(j, block, slot, chip):
        return remote(kv_v.at[j, block], kv_v.at[j, block], rel_sem.at[j, slot], kv_sem.at[j, block], dev(chip, s))

    def kv_wait(j, block):
        remote(kv_v.at[j, block], kv_v.at[j, block], kvp_sem.at[0], kv_sem.at[j, block], (dp, mate)).wait_recv()

    def o_copy(j):
        return remote(oo_v.at[j, 1 - s], or_v.at[j], o_sem.at[0, j], o_sem.at[1, j], (dp, mate))

    sends_down = jnp.logical_or(first, jnp.logical_and(c == 1, s == 1))
    second = c == 1
    even, odd = s == 0, s == 1
    third = c == 2

    def both(a, b):
        return jnp.logical_and(a, b)

    routes = ((0, 3, down), (1, 0, up), (2, 2, up), (3, 1, down))

    def relay_now(j, chips):
        for chip, block, to in routes[chips]:
            @pl.when(c == chip)
            def _():
                kv_wait(j, block)
                relay(j, block, 0, to).start()

    loads[0].wait()
    loads[1].wait()
    loads[5].start()
    wq_load(0).start()
    gain = jnp.concatenate([ln_v[k:k + 1, :] for k in range(feats // head)], axis=1).astype(F32)
    step = 64

    def norm_rows(r, _):
        x = x_v[0, pl.ds(pl.multiple_of(r * step, step), step), :].astype(F32)
        inv = lax.rsqrt(jnp.mean(x * x, axis=-1, keepdims=True) + EPS)
        h_v[s, pl.ds(pl.multiple_of(r * step, step), step), :] = (x * inv * gain).astype(BF16)
        return 0

    lax.fori_loop(0, rows // step, norm_rows, 0)
    pl.semaphore_wait(barrier, 1 + 2 * CORES)
    h_copy.start()
    for load in loads[2:5]:
        load.wait()
    k_gain = kg_v[...].astype(F32).reshape(1, head)

    def norm_rope(t, g, cos, sin):
        t = t * lax.rsqrt(jnp.mean(t * t, axis=-1, keepdims=True) + EPS) * g
        return (t * cos + pltpu.roll(t, head // 2, 1) * sin).astype(BF16)

    def finish_kv(j):
        for core in range(CORES):
            pk_v[j, core, 0] = norm_rope(raw_v[j, :rows, core * head:(core + 1) * head], k_gain, rope_v[0], rope_v[1])
            pk_v[j, core, 1] = raw_v[j, :rows, kvw + core * head:kvw + (core + 1) * head].T.astype(BF16)

    def send_up(j):
        for core in range(CORES):
            to_up(j, core).start()

    def send_down(j):
        for core in range(CORES):
            to_down(j, core).start()

    def send(when, *calls):
        @pl.when(when)
        def _():
            for call, j in calls:
                call(j)

    def send_kv(j):
        if j == 0:
            send(jnp.logical_or(third, both(c < 2, even)), (send_up, 0))
            send(both(c < 2, odd), (send_down, 0))
        else:
            send(both(first, even), (send_down, 0), (send_up, 1))
            send(both(second, odd), (send_up, 0), (send_down, 1))
            send(both(third, even), (send_up, 1))
        to_mate(j).start()
        kv_v[j, mine] = pk_v[j, s]

    def send_rest(part):
        if part == 0:
            send(both(first, odd), (send_up, 0), (send_up, 1), (send_down, 1))
            send(both(second, even), (send_up, 1))
        else:
            relay_now(0, slice(0, 4))
            send(both(first, even), (send_down, 1))
            send(jnp.logical_or(both(second, odd), both(third, odd)), (send_up, 1))

    for j in range(halves):
        wkv_load(j, 0).wait()
        wkv_load(j, 1).wait()
        raw_v[j, :rows, :2 * kvw] = jnp.dot(h_v[s], wkv_v[j], preferred_element_type=F32)
        finish_kv(j)
        if j == 0:
            for i in range(1, n_wq):
                wq_load(i).start()
        send_kv(j)

    h_copy.wait_recv()

    loads[5].wait()
    q_gain = jnp.broadcast_to(qg_v[...].astype(F32), (head, head)).T
    q_gain = jnp.concatenate([q_gain] * CORES, axis=1)

    def turn(t):
        return jnp.concatenate([t[head // 2:], t[:head // 2]], axis=0)

    ropet_v[0] = ropet_v[0] * q_gain
    ropet_v[1] = ropet_v[1] * turn(q_gain)

    def finish_q(i):
        for g in range(qcols // head):
            t = raw_v[i % 2, :, g * head:(g + 1) * head].T
            t = t * lax.rsqrt(jnp.mean(t * t, axis=0, keepdims=True) + EPS)
            q_v[i * (qcols // head) + g] = (t * ropet_v[0] + turn(t) * ropet_v[1]).astype(BF16)

    for i in range(n_wq):
        wq_load(i).wait()
        if i == n_wq - 1:
            for n in range(n_wo):
                wo_load(n).start()
        raw_v[i % 2] = jnp.dot(h_v[...].reshape(pair, feats), wq_v[i], preferred_element_type=F32)
        if i:
            finish_q(i - 1)
        if i + 1 < n_wq:
            send_rest(0)
    def attend(j, blocks, diagonal):
        keys = [kv_v[j, pl.ds(block * CORES, CORES), 0].reshape(pair, head) for block in blocks]
        vals = jnp.concatenate([kv_v[j, block * CORES + core, 1] for block in blocks for core in range(CORES)], axis=1)
        span = len(blocks) * pair
        if diagonal:
            key = lax.broadcasted_iota(jnp.int32, (rows, rows), 0)
            row = lax.broadcasted_iota(jnp.int32, (rows, rows), 1)
            seen = key <= row

            def hide(sc):
                return jnp.where(seen, sc, -jnp.inf)

        def score(g):
            i = j * group + g
            top = None
            if diagonal:
                early = jnp.dot(keys[0][:rows], q_v[i], preferred_element_type=F32)
                early = jnp.concatenate([hide(early[:, :rows]), early[:, rows:]], axis=1)
                late = hide(jnp.dot(keys[0][rows:], q_v[i, :, rows:], preferred_element_type=F32))
                s_v[i, :rows] = early
                s_v[i, rows:pair, rows:] = late
                top = jnp.max(early, axis=0, keepdims=True)
                both = jnp.maximum(top[:, rows:], jnp.max(late, axis=0, keepdims=True))
                return jnp.concatenate([top[:, :rows], both], axis=1) * scale
            for n in range(len(blocks)):
                sc = jnp.dot(keys[n], q_v[i], preferred_element_type=F32)
                s_v[i, n * pair:(n + 1) * pair] = sc
                best = jnp.max(sc, axis=0, keepdims=True) * scale
                top = best if top is None else jnp.maximum(top, best)
            return top

        def mix(g, new):
            i = j * group + g
            if not diagonal:
                old = m_v[i]
                new = jnp.maximum(old, new)
            m_v[i] = new
            if diagonal:
                early = jnp.exp2(s_v[i, :rows] * scale - new)
                late = jnp.exp2(s_v[i, rows:pair, rows:] * scale - new[:, rows:])
                total = jnp.sum(early, axis=0, keepdims=True)
                total = jnp.concatenate([total[:, :rows], total[:, rows:] + jnp.sum(late, axis=0, keepdims=True)], axis=1)
                probs = jnp.concatenate([early, jnp.concatenate([jnp.zeros_like(late), late], axis=1)], axis=0)
            else:
                probs = jnp.exp2(s_v[i, :span] * scale - new)
                total = jnp.sum(probs, axis=0, keepdims=True)
            mixed = jnp.dot(vals, probs.astype(BF16), preferred_element_type=F32)
            if diagonal:
                l_v[i] = total
                acc_v[i] = mixed
            else:
                fade = jnp.exp2(old - new)
                l_v[i] = l_v[i] * fade + total
                acc_v[i] = acc_v[i] * fade + mixed

        tops = [score(g) for g in range(group)]
        for g in range(group):
            mix(g, tops[g])

    def project_out(parts, fresh):
        for n in range(feats // ocols):
            cols = slice(n * ocols, (n + 1) * ocols)
            total = sum(jnp.dot(o_ref[...], wo_v[i, :, cols], preferred_element_type=F32) for o_ref, i in parts)
            y_v[:, cols] = total if fresh else y_v[:, cols] + total

    for j in range(halves):
        kv_wait(j, mate)
    send_rest(1)
    finish_q(n_wq - 1)
    for j in range(halves):
        attend(j, [c], True)

    relay_now(1, slice(0, 2))

    block = c - lax.div(c, 2) - 1

    def one_half(j, _):
        @pl.when(third)
        def _():
            kv_wait(j, 3)
            attend(j, [c - 1], False)

            @pl.when(j == 0)
            def _():
                kv_wait(1, 2)
                relay(1, 2, 0, up).start()

        @pl.when(last)
        def _():
            for piece in (4, 5, 0):
                kv_wait(j, piece)
            attend(j, [c - 1, 0], False)

            @pl.when(j == 0)
            def _():
                kv_wait(1, 1)
                relay(1, 1, 0, down).start()

        for chip, pieces in ((1, (1,)), (2, (0, 1)), (3, (2, 3))):
            @pl.when(c == chip)
            def _():
                for piece in pieces:
                    kv_wait(j, piece)

        @pl.when(c > 0)
        def _():
            attend(j, [block], False)

        for g in range(group):
            i = j * group + g
            o = acc_v[i] * (1.0 / l_v[i])
            for core in range(CORES):
                oo_v[j, core, :, g * head:(g + 1) * head] = o[:, core * rows:(core + 1) * rows].T.astype(BF16)
        o_copy(j).start()
        return 0

    lax.fori_loop(0, halves, one_half, 0)
    for i in range(n_wo):
        wo_load(i).wait()
    o_copy(0).wait_recv()
    project_out(((oo_v.at[0, s], s), (or_v.at[0], 1 - s), (oo_v.at[1, s], CORES + s)), True)
    o_copy(1).wait_recv()
    project_out(((or_v.at[1], CORES + 1 - s),), False)

    h_copy.wait_send()
    for j in range(halves):
        to_mate(j).wait_send()
        o_copy(j).wait_send()
        for core in range(CORES):
            @pl.when(jnp.logical_not(last))
            def _():
                to_up(j, core).wait_send()

            @pl.when(sends_down)
            def _():
                to_down(j, core).wait_send()

        for chip, block, to in routes:
            @pl.when(c == chip)
            def _():
                relay(j, block, 0, to).wait_send()


def solution(mesh):
    group_size = mesh.shape['sp']
    assert group_size == CORES * CHIPS

    def device_step(hidden, ln_gain, w_q, w_k, w_v, w_o, q_gain, k_gain):
        rows, feats = hidden.shape
        head = q_gain.shape[0]
        kv_heads = w_k.shape[1] // head
        q_heads = w_q.shape[1] // head
        halves = kv_heads // CORES
        group = q_heads // kv_heads
        width = group * head
        pair = CORES * rows
        qcols = width
        n_wq = halves * width // qcols
        tables = np.stack(rope_tables(group_size * rows, head))
        by_device = tables.reshape(2, group_size, rows, head).transpose(1, 0, 2, 3)
        by_chip = tables.reshape(2, CHIPS, pair, head).transpose(1, 0, 3, 2)
        dma = pltpu.SemaphoreType.DMA
        any_spec = pl.BlockSpec(memory_space=pl.ANY)
        scratch = [
            pltpu.VMEM((1, rows, feats), BF16),
            pltpu.VMEM((feats // head, head), BF16),
            pltpu.VMEM((1, head), BF16),
            pltpu.VMEM((1, head), BF16),
            pltpu.VMEM((2, rows, head), F32),
            pltpu.VMEM((2, head, pair), F32),
            pltpu.VMEM((halves, feats, 2 * CORES * head), BF16),
            pltpu.VMEM((n_wq, feats, qcols), BF16),
            pltpu.VMEM((kv_heads, width, feats), BF16),
            pltpu.VMEM((CORES, rows, feats), BF16),
            pltpu.VMEM((halves, CORES, 2, rows, head), BF16),
            pltpu.VMEM((halves, group_size, 2, rows, head), BF16),
            pltpu.VMEM((2, pair, qcols), F32),
            pltpu.VMEM((halves * group, head, pair), BF16),
            pltpu.VMEM((halves * group, 2 * pair, pair), F32),
            pltpu.VMEM((halves * group, head, pair), F32),
            pltpu.VMEM((halves * group, 1, pair), F32),
            pltpu.VMEM((halves * group, 1, pair), F32),
            pltpu.VMEM((halves, CORES, rows, width), BF16),
            pltpu.VMEM((halves, rows, width), BF16),
            dma((6,)), dma((halves, 2)), dma((n_wq,)), dma((kv_heads,)), dma((2,)),
            dma((halves,)), dma((halves, CORES)), dma((halves, CORES)), dma((halves, CORES)),
            dma((halves, group_size)), dma((2, halves)),
        ]
        mixed = pl.pallas_call(
            kernel,
            out_shape=pltpu.VMEM((rows, feats), F32),
            in_specs=[any_spec] * 10,
            out_specs=pl.BlockSpec(memory_space=pltpu.VMEM),
            scratch_shapes=scratch,
            compiler_params=pltpu.CompilerParams(
                collective_id=0, has_side_effects=True, vmem_limit_bytes=56 * 2 ** 20
            ),
            name="attention_block",
        )(hidden, ln_gain.reshape(-1, head), w_q, w_k, w_v, w_o, q_gain.reshape(1, -1), k_gain.reshape(1, -1),
          jnp.asarray(by_device), jnp.asarray(by_chip))
        return (hidden.astype(F32) + mixed).astype(BF16)

    row_spec = P(('dp', 'sp'), None)
    return jax.shard_map(device_step, mesh=mesh, in_specs=(row_spec, P(), P(), P(), P(), P(), P(), P()), out_specs=row_spec, check_vma=False)
```

```python
import functools
import numpy as np
import jax
import jax.numpy as jnp
from jax import lax
from jax.experimental import pallas as pl
from jax.experimental.pallas import tpu as pltpu
from jax.sharding import PartitionSpec as P

EPS = 1e-6
THETA = 1000000.0
LOG2E = 1.4426950408889634
MESH = pl.DeviceIdType.MESH
CORES = 2
CHIPS = 4
BF16 = jnp.bfloat16
F32 = jnp.float32


def rope_tables(rows, head_dim):
    half = head_dim // 2
    inv_freq = np.power(np.float32(THETA), -(np.arange(half, dtype=np.float32) * np.float32(2.0 / head_dim)))
    angles = np.arange(rows, dtype=np.float32)[:, None] * inv_freq.astype(np.float32)[None, :]
    cos = np.cos(angles.astype(np.float64)).astype(np.float32)
    sin = np.sin(angles.astype(np.float64)).astype(np.float32)
    return np.concatenate([cos, cos], axis=1), np.concatenate([-sin, sin], axis=1)


def kernel(x_hbm, ln_hbm, wq_hbm, wk_hbm, wv_hbm, wo_hbm, qg_hbm, kg_hbm, rope_hbm, ropet_hbm, out_v,
           x_v, ln_v, qg_v, kg_v, rope_v, ropet_v, wkv_v, wq_v, wo_v, h_v, pk_v, kv_v, raw_v, q_v, s_v, acc_v, m_v, l_v,
           oo_v, or_v, y_v,
           ld_sem, wkv_sem, wq_sem, wo_sem, h_sem, send_sem, kv_sem, o_sem):
    rows, feats = x_v.shape[1], x_v.shape[2]
    head = rope_v.shape[-1]
    pair = CORES * rows
    halves = wkv_v.shape[0]
    group = q_v.shape[0] // halves
    width = group * head
    scale = head ** -0.5 * LOG2E
    qcols = wq_v.shape[2]
    qparts = width // qcols
    ocols = 512

    dp = lax.axis_index("dp")
    sp = lax.axis_index("sp")
    c = lax.div(sp, CORES)
    s = lax.rem(sp, CORES)
    mate = c * CORES + (1 - s)
    up = lax.rem(c + 1, CHIPS)
    down = lax.rem(c + CHIPS - 1, CHIPS)
    first, last = c == 0, c == CHIPS - 1
    mine = c * CORES + s

    def dev(chip, core):
        return (dp, chip * CORES + core)

    loads = [
        pltpu.make_async_copy(x_hbm, x_v.at[0], ld_sem.at[0]),
        pltpu.make_async_copy(ln_hbm, ln_v, ld_sem.at[1]),
        pltpu.make_async_copy(qg_hbm, qg_v, ld_sem.at[2]),
        pltpu.make_async_copy(kg_hbm, kg_v, ld_sem.at[3]),
        pltpu.make_async_copy(rope_hbm.at[c * CORES + s], rope_v, ld_sem.at[4]),
        pltpu.make_async_copy(ropet_hbm.at[c], ropet_v, ld_sem.at[5]),
    ]
    kvw = CORES * head

    def wkv_load(j, which):
        src = (wk_hbm, wv_hbm)[which]
        return pltpu.make_async_copy(src.at[:, pl.ds(j * kvw, kvw)], wkv_v.at[j, :, pl.ds(which * kvw, kvw)], wkv_sem.at[j])

    halfq = qcols // 2

    def wq_load(i):
        if i < 2:
            col = s * width + i * halfq
            return pltpu.make_async_copy(wq_hbm.at[:, pl.ds(pl.multiple_of(col, halfq), halfq)], wq_v.at[0, :, pl.ds(i * halfq, halfq)], wq_sem.at[i])
        col = (CORES * (i - 1) + s) * width
        return pltpu.make_async_copy(wq_hbm.at[:, pl.ds(pl.multiple_of(col, qcols), qcols)], wq_v.at[i - 1], wq_sem.at[i])

    def wo_load(i, sem):
        return pltpu.make_async_copy(wo_hbm.at[pl.ds(pl.multiple_of(i * width, width), width)], wo_v.at[i], sem)

    n_wq = halves * qparts
    n_wo = CORES * halves
    stages = [wkv_load(j, which) for j in range(halves) for which in range(2)]
    for load in loads[:5] + stages[:2]:
        load.start()

    barrier = pltpu.get_barrier_semaphore()
    pl.semaphore_signal(barrier, inc=1, device_id=(dp, mate), device_id_type=MESH)
    for chip in (up, down):
        for core in range(CORES):
            pl.semaphore_signal(barrier, inc=1, device_id=dev(chip, core), device_id_type=MESH)

    def remote(src, dst, send, recv, to):
        return pltpu.make_async_remote_copy(src_ref=src, dst_ref=dst, send_sem=send, recv_sem=recv, device_id=to, device_id_type=MESH)

    h_copy = remote(h_v.at[s], h_v.at[s], h_sem.at[0], h_sem.at[1], (dp, mate))

    def to_mate(j):
        return remote(pk_v.at[j, 1 - s], kv_v.at[j, mine], send_sem.at[0], kv_sem.at[j, mine], (dp, mate))

    def to_up(j, core):
        return remote(pk_v.at[j, core], kv_v.at[j, mine], send_sem.at[1], kv_sem.at[j, mine], dev(up, core))

    def to_down(j, core):
        return remote(pk_v.at[j, core], kv_v.at[j, mine], send_sem.at[2], kv_sem.at[j, mine], dev(down, core))

    def relay(j, block, chip):
        return remote(kv_v.at[j, block], kv_v.at[j, block], send_sem.at[3], kv_sem.at[j, block], dev(chip, s))

    def kv_wait(j, block):
        remote(kv_v.at[j, block], kv_v.at[j, block], send_sem.at[0], kv_sem.at[j, block], (dp, mate)).wait_recv()

    def o_copy(j, part=None):
        theirs = 1 - s
        if part is None:
            return remote(oo_v.at[j, theirs], or_v.at[j], o_sem.at[0], o_sem.at[1 + j], (dp, mate))
        return remote(oo_v.at[j, theirs, part], or_v.at[j, part], o_sem.at[0], o_sem.at[1 + j], (dp, mate))

    sends_down = jnp.logical_or(first, jnp.logical_and(c == 1, s == 1))
    second = c == 1
    even, odd = s == 0, s == 1
    third = c == 2

    def both(a, b):
        return jnp.logical_and(a, b)

    routes = ((0, 3, down), (1, 0, up), (2, 2, up), (3, 1, down))

    def relay_now(j, chips):
        for chip, block, to in routes[chips]:
            @pl.when(c == chip)
            def _():
                kv_wait(j, block)
                relay(j, block, to).start()

    loads[0].wait()
    loads[1].wait()
    for load in stages[2:]:
        load.start()
    gain = jnp.concatenate([ln_v[k:k + 1, :] for k in range(feats // head)], axis=1).astype(F32)
    step = 64

    def norm_rows(r, _):
        x = x_v[0, pl.ds(pl.multiple_of(r * step, step), step), :].astype(F32)
        inv = lax.rsqrt(jnp.mean(x * x, axis=-1, keepdims=True) + EPS)
        h_v[s, pl.ds(pl.multiple_of(r * step, step), step), :] = (x * inv * gain).astype(BF16)
        return 0

    lax.fori_loop(0, rows // step, norm_rows, 0)
    wq_load(0).start()
    loads[5].start()
    pl.semaphore_wait(barrier, 1 + 2 * CORES)
    h_copy.start()
    for load in loads[2:5]:
        load.wait()
    k_gain = kg_v[...].astype(F32).reshape(1, head)

    def norm_rope(t, g, cos, sin):
        t = t * lax.rsqrt(jnp.mean(t * t, axis=-1, keepdims=True) + EPS) * g
        return (t * cos + pltpu.roll(t, head // 2, 1) * sin).astype(BF16)

    def finish_kv(j):
        for core in range(CORES):
            pk_v[j, core, 0] = norm_rope(raw_v[j, :rows, core * head:(core + 1) * head], k_gain, rope_v[0], rope_v[1])
            pk_v[j, core, 1] = raw_v[j, :rows, kvw + core * head:kvw + (core + 1) * head].T.astype(BF16)

    def send_up(j):
        for core in range(CORES):
            to_up(j, core).start()

    def send_down(j):
        for core in range(CORES):
            to_down(j, core).start()

    def send(when, *calls):
        @pl.when(when)
        def _():
            for call, j in calls:
                call(j)

    def send_kv(j):
        if j == 0:
            send(jnp.logical_or(third, both(c < 2, even)), (send_up, 0))
            send(both(c < 2, odd), (send_down, 0))
        else:
            send(both(first, even), (send_down, 0), (send_up, 1))
            send(both(second, odd), (send_up, 0), (send_down, 1))
            send(both(third, even), (send_up, 1))
        to_mate(j).start()
        kv_v[j, mine] = pk_v[j, s]

    def send_rest(part):
        if part == 0:
            send(both(first, odd), (send_up, 0), (send_up, 1), (send_down, 1))
            send(both(second, even), (send_up, 1))
        else:
            relay_now(0, slice(0, 4))
            send(both(first, even), (send_down, 1))
            send(jnp.logical_or(both(second, odd), both(third, odd)), (send_up, 1))

    for j in range(halves):
        pltpu.make_async_copy(wkv_v.at[j], wkv_v.at[j], wkv_sem.at[j]).wait()
        if j == 0:
            wq_load(1).start()
        raw_v[j, :rows, :2 * kvw] = jnp.dot(h_v[s], wkv_v[j], preferred_element_type=F32)
        finish_kv(j)
        if j == 0:
            wq_load(2).start()
        send_kv(j)

    h_copy.wait_recv()

    loads[5].wait()
    q_gain = jnp.broadcast_to(qg_v[...].astype(F32), (head, head)).T
    q_gain = jnp.concatenate([q_gain] * CORES, axis=1)

    def turn(t):
        return jnp.concatenate([t[head // 2:], t[:head // 2]], axis=0)

    ropet_v[0] = ropet_v[0] * q_gain
    ropet_v[1] = ropet_v[1] * turn(q_gain)

    def finish_q(i):
        for g in range(qcols // head):
            t = raw_v[i % 2, :, g * head:(g + 1) * head].T
            t = t * lax.rsqrt(jnp.mean(t * t, axis=0, keepdims=True) + EPS)
            q_v[i * (qcols // head) + g] = (t * ropet_v[0] + turn(t) * ropet_v[1]).astype(BF16)

    for i in range(2):
        wq_load(i).wait()
        cols = slice(i * halfq, (i + 1) * halfq)
        raw_v[0, :, cols] = jnp.dot(h_v[...].reshape(pair, feats), wq_v[0, :, cols], preferred_element_type=F32)
    send_rest(0)
    for i in range(1, n_wq):
        wq_load(i + 1).wait()
        wo_load(s, wo_sem.at[0]).start()
        for n in (1 - s, CORES + s, CORES + 1 - s):
            wo_load(n, wo_sem.at[1]).start()
        raw_v[i] = jnp.dot(h_v[...].reshape(pair, feats), wq_v[i], preferred_element_type=F32)
        finish_q(i - 1)

    def attend(j, pieces, diagonal):
        keys = [kv_v[j, piece, 0] for piece in pieces]
        keys = [jnp.concatenate(keys[n:n + CORES], axis=0) for n in range(0, len(pieces), CORES)]
        vals = jnp.concatenate([kv_v[j, piece, 1] for piece in pieces], axis=1)
        span = len(pieces) * rows
        if diagonal:
            key = lax.broadcasted_iota(jnp.int32, (rows, rows), 0)
            row = lax.broadcasted_iota(jnp.int32, (rows, rows), 1)
            seen = key <= row

            def hide(sc):
                return jnp.where(seen, sc, -jnp.inf)

        def score(g):
            i = j * group + g
            top = None
            if diagonal:
                early = jnp.dot(keys[0][:rows], q_v[i], preferred_element_type=F32)
                early = jnp.concatenate([hide(early[:, :rows]), early[:, rows:]], axis=1)
                late = hide(jnp.dot(keys[0][rows:], q_v[i, :, rows:], preferred_element_type=F32))
                s_v[i, :rows] = early
                s_v[i, rows:pair, rows:] = late
                top = jnp.max(early, axis=0, keepdims=True)
                both = jnp.maximum(top[:, rows:], jnp.max(late, axis=0, keepdims=True))
                return jnp.concatenate([top[:, :rows], both], axis=1) * scale
            for n in range(len(keys)):
                sc = jnp.dot(keys[n], q_v[i], preferred_element_type=F32)
                s_v[i, n * pair:(n + 1) * pair] = sc
                best = jnp.max(sc, axis=0, keepdims=True) * scale
                top = best if top is None else jnp.maximum(top, best)
            return top

        def mix(g, new):
            i = j * group + g
            if not diagonal:
                old = m_v[i]
                new = jnp.maximum(old, new)
            m_v[i] = new
            if diagonal:
                early = jnp.exp2(s_v[i, :rows] * scale - new)
                late = jnp.exp2(s_v[i, rows:pair, rows:] * scale - new[:, rows:])
                total = jnp.sum(early, axis=0, keepdims=True)
                total = jnp.concatenate([total[:, :rows], total[:, rows:] + jnp.sum(late, axis=0, keepdims=True)], axis=1)
                probs = jnp.concatenate([early, jnp.concatenate([jnp.zeros_like(late), late], axis=1)], axis=0)
            else:
                probs = jnp.exp2(s_v[i, :span] * scale - new)
                total = jnp.sum(probs, axis=0, keepdims=True)
            mixed = jnp.dot(vals, probs.astype(BF16), preferred_element_type=F32)
            if diagonal:
                l_v[i] = total
                acc_v[i] = mixed
            else:
                fade = jnp.exp2(old - new)
                l_v[i] = l_v[i] * fade + total
                acc_v[i] = acc_v[i] * fade + mixed

        tops = [score(g) for g in range(group)]
        for g in range(group):
            mix(g, tops[g])

    def project(part, cols):
        o_ref, i = part
        return jnp.dot(jnp.concatenate([o_ref[0], o_ref[1]], axis=1), wo_v[i, :, cols], preferred_element_type=F32)

    for j in range(halves):
        kv_wait(j, mate)
    send_rest(1)
    finish_q(n_wq - 1)
    for j in range(halves):
        attend(j, [c * CORES, c * CORES + 1], True)

    relay_now(1, slice(0, 2))

    @pl.when(last)
    def _():
        for piece in (4, 5, 0):
            kv_wait(0, piece)
        attend(0, (4, 5, 0, 1), False)
        kv_wait(1, 1)
        relay(1, 1, down).start()

    def one_step(n, _):
        is3 = lax.div(c, 3)
        is2 = lax.div(c, 2) - is3
        half = lax.div(n, 2)
        odd_step = lax.rem(n, 2)
        even_step = 1 - odd_step
        j = half + is3 * lax.div(3 - n, 3)
        piece0 = is3 * (even_step * (4 + half) + odd_step * 2) + is2 * 2 * even_step
        piece1 = is3 * (even_step * (1 - half) + odd_step * 3) + is2 * (2 * even_step + 1) + (1 - is3 - is2)

        @pl.when(jnp.logical_or(both(third, n % 2 == 1), last))
        def _():
            kv_wait(j, piece0)

        @pl.when(jnp.logical_or(jnp.logical_or(both(second, n % 2 == 1), third), both(last, n > 0)))
        def _():
            kv_wait(j, piece1)

        @pl.when(jnp.logical_or(c > 1, both(second, n % 2 == 1)))
        def _():
            attend(j, (piece0, piece1), False)

        @pl.when(both(third, n == 0))
        def _():
            kv_wait(1, 2)
            relay(1, 2, up).start()

        @pl.when(n % 2 == 1)
        def _():
            for part in range(2):
                for g in range(group // 2):
                    i = half * group + part * (group // 2) + g
                    o = acc_v[i] * (1.0 / l_v[i])
                    for core in range(CORES):
                        oo_v[half, core, part, :, g * head:(g + 1) * head] = o[:, core * rows:(core + 1) * rows].T.astype(BF16)
                o_copy(half, part).start()

        @pl.when(n == 1)
        def _():
            wo_load(s, wo_sem.at[0]).wait()
            for k in range(feats // ocols):
                cols = slice(k * ocols, (k + 1) * ocols)
                y_v[:, cols] = x_v[0, :, cols].astype(F32) + project((oo_v.at[0, s], s), cols)

        return 0

    lax.fori_loop(0, 2 * halves, one_step, 0)
    pltpu.make_async_copy(wo_v.at[pl.ds(1, n_wo - 1)], wo_v.at[pl.ds(1, n_wo - 1)], wo_sem.at[1]).wait()
    o_copy(0).wait_recv()
    for k in range(feats // ocols):
        cols = slice(k * ocols, (k + 1) * ocols)
        y_v[:, cols] += project((or_v.at[0], 1 - s), cols) + project((oo_v.at[1, s], CORES + s), cols)
    o_copy(1).wait_recv()
    for k in range(feats // ocols):
        cols = slice(k * ocols, (k + 1) * ocols)
        out_v[:, cols] = (y_v[:, cols] + project((or_v.at[1], CORES + 1 - s), cols)).astype(BF16)

    h_copy.wait_send()
    theirs = 1 - s
    remote(pk_v.at[:, theirs], kv_v.at[:, mine], send_sem.at[0], kv_sem.at[0, 0], (dp, mate)).wait_send()
    remote(oo_v.at[:, theirs], or_v, o_sem.at[0], o_sem.at[1], (dp, mate)).wait_send()

    def sent(sem):
        remote(pk_v, kv_v.at[:, pl.ds(0, CORES)], sem, kv_sem.at[0, 0], (dp, mate)).wait_send()

    pl.when(jnp.logical_not(last))(functools.partial(sent, send_sem.at[1]))
    pl.when(sends_down)(functools.partial(sent, send_sem.at[2]))
    remote(kv_v.at[:, 0], kv_v.at[:, 0], send_sem.at[3], kv_sem.at[0, 0], (dp, mate)).wait_send()


def solution(mesh):
    group_size = mesh.shape['sp']
    assert group_size == CORES * CHIPS

    def device_step(hidden, ln_gain, w_q, w_k, w_v, w_o, q_gain, k_gain):
        rows, feats = hidden.shape
        head = q_gain.shape[0]
        kv_heads = w_k.shape[1] // head
        q_heads = w_q.shape[1] // head
        halves = kv_heads // CORES
        group = q_heads // kv_heads
        width = group * head
        pair = CORES * rows
        qcols = width
        n_wq = halves * width // qcols
        tables = np.stack(rope_tables(group_size * rows, head))
        by_device = tables.reshape(2, group_size, rows, head).transpose(1, 0, 2, 3)
        by_chip = tables.reshape(2, CHIPS, pair, head).transpose(1, 0, 3, 2)
        dma = pltpu.SemaphoreType.DMA
        any_spec = pl.BlockSpec(memory_space=pl.ANY)
        scratch = [
            pltpu.VMEM((1, rows, feats), BF16),
            pltpu.VMEM((feats // head, head), BF16),
            pltpu.VMEM((1, head), BF16),
            pltpu.VMEM((1, head), BF16),
            pltpu.VMEM((2, rows, head), F32),
            pltpu.VMEM((2, head, pair), F32),
            pltpu.VMEM((halves, feats, 2 * CORES * head), BF16),
            pltpu.VMEM((n_wq, feats, qcols), BF16),
            pltpu.VMEM((kv_heads, width, feats), BF16),
            pltpu.VMEM((CORES, rows, feats), BF16),
            pltpu.VMEM((halves, CORES, 2, rows, head), BF16),
            pltpu.VMEM((halves, group_size, 2, rows, head), BF16),
            pltpu.VMEM((2, pair, qcols), F32),
            pltpu.VMEM((halves * group, head, pair), BF16),
            pltpu.VMEM((halves * group, 2 * pair, pair), F32),
            pltpu.VMEM((halves * group, head, pair), F32),
            pltpu.VMEM((halves * group, 1, pair), F32),
            pltpu.VMEM((halves * group, 1, pair), F32),
            pltpu.VMEM((halves, CORES, 2, rows, width // 2), BF16),
            pltpu.VMEM((halves, 2, rows, width // 2), BF16),
            pltpu.VMEM((rows, feats), F32),
            dma((6,)), dma((halves,)), dma((n_wq + 1,)), dma((2,)), dma((2,)), dma((4,)), dma((halves, group_size)), dma((1 + halves,)),
        ]
        mixed = pl.pallas_call(
            kernel,
            out_shape=pltpu.VMEM((rows, feats), BF16),
            in_specs=[any_spec] * 10,
            out_specs=pl.BlockSpec(memory_space=pltpu.VMEM),
            scratch_shapes=scratch,
            compiler_params=pltpu.CompilerParams(
                collective_id=0, has_side_effects=True, vmem_limit_bytes=56 * 2 ** 20
            ),
            name="attention_block",
        )(hidden, ln_gain.reshape(-1, head), w_q, w_k, w_v, w_o, q_gain.reshape(1, -1), k_gain.reshape(1, -1),
          jnp.asarray(by_device), jnp.asarray(by_chip))
        return mixed

    row_spec = P(('dp', 'sp'), None)
    return jax.shard_map(device_step, mesh=mesh, in_specs=(row_spec, P(), P(), P(), P(), P(), P(), P()), out_specs=row_spec, check_vma=False)
```

```python
import functools
import numpy as np
import jax
import jax.numpy as jnp
from jax import lax
from jax.experimental import pallas as pl
from jax.experimental.pallas import tpu as pltpu
from jax.sharding import PartitionSpec as P

EPS = 1e-6
THETA = 1000000.0
LOG2E = 1.4426950408889634
MESH = pl.DeviceIdType.MESH
CORES = 2
CHIPS = 4
BF16 = jnp.bfloat16
F32 = jnp.float32


def rope_tables(rows, head_dim):
    half = head_dim // 2
    inv_freq = np.power(np.float32(THETA), -(np.arange(half, dtype=np.float32) * np.float32(2.0 / head_dim)))
    angles = np.arange(rows, dtype=np.float32)[:, None] * inv_freq.astype(np.float32)[None, :]
    cos = np.cos(angles.astype(np.float64)).astype(np.float32)
    sin = np.sin(angles.astype(np.float64)).astype(np.float32)
    return np.concatenate([cos, cos], axis=1), np.concatenate([-sin, sin], axis=1)


def kernel(x_hbm, ln_hbm, wq_hbm, wk_hbm, wv_hbm, wo_hbm, qg_hbm, kg_hbm, rope_hbm, ropet_hbm, out_v,
           x_v, ln_v, qg_v, kg_v, rope_v, ropet_v, wkv_v, wq_v, wo_v, h_v, pk_v, kv_v, raw_v, q_v, s_v, acc_v, m_v, l_v,
           oo_v, or_v, y_v,
           ld_sem, wkv_sem, wq_sem, wo_sem, h_sem, send_sem, kv_sem, o_sem):
    rows, feats = x_v.shape[1], x_v.shape[2]
    head = rope_v.shape[-1]
    pair = CORES * rows
    halves = wkv_v.shape[0]
    group = q_v.shape[0] // halves
    width = group * head
    scale = head ** -0.5 * LOG2E
    qcols = wq_v.shape[2]
    qparts = width // qcols
    ocols = 512

    dp = lax.axis_index("dp")
    sp = lax.axis_index("sp")
    c = lax.div(sp, CORES)
    s = lax.rem(sp, CORES)
    mate = c * CORES + (1 - s)
    up = lax.rem(c + 1, CHIPS)
    down = lax.rem(c + CHIPS - 1, CHIPS)
    first, last = c == 0, c == CHIPS - 1
    mine = c * CORES + s

    def dev(chip, core):
        return (dp, chip * CORES + core)

    loads = [
        pltpu.make_async_copy(x_hbm, x_v.at[0], ld_sem.at[0]),
        pltpu.make_async_copy(ln_hbm, ln_v, ld_sem.at[1]),
        pltpu.make_async_copy(qg_hbm, qg_v, ld_sem.at[2]),
        pltpu.make_async_copy(kg_hbm, kg_v, ld_sem.at[3]),
        pltpu.make_async_copy(rope_hbm.at[c * CORES + s], rope_v, ld_sem.at[4]),
        pltpu.make_async_copy(ropet_hbm.at[c], ropet_v, ld_sem.at[5]),
    ]
    kvw = CORES * head

    def wkv_load(j, which):
        src = (wk_hbm, wv_hbm)[which]
        return pltpu.make_async_copy(src.at[:, pl.ds(j * kvw, kvw)], wkv_v.at[j, :, pl.ds(which * kvw, kvw)], wkv_sem.at[j])

    halfq = qcols // 2

    def wq_load(i):
        if i < 2:
            col = s * width + i * halfq
            return pltpu.make_async_copy(wq_hbm.at[:, pl.ds(pl.multiple_of(col, halfq), halfq)], wq_v.at[0, :, pl.ds(i * halfq, halfq)], wq_sem.at[i])
        col = (CORES * (i - 1) + s) * width
        return pltpu.make_async_copy(wq_hbm.at[:, pl.ds(pl.multiple_of(col, qcols), qcols)], wq_v.at[i - 1], wq_sem.at[i])

    def wo_load(i, sem):
        return pltpu.make_async_copy(wo_hbm.at[pl.ds(pl.multiple_of(i * width, width), width)], wo_v.at[i], sem)

    n_wq = halves * qparts
    n_wo = CORES * halves
    stages = [wkv_load(j, which) for j in range(halves) for which in range(2)]
    for load in loads[:5] + stages[:2]:
        load.start()

    barrier = pltpu.get_barrier_semaphore()
    pl.semaphore_signal(barrier, inc=1, device_id=(dp, mate), device_id_type=MESH)
    for chip in (up, down):
        for core in range(CORES):
            pl.semaphore_signal(barrier, inc=1, device_id=dev(chip, core), device_id_type=MESH)

    def remote(src, dst, send, recv, to):
        return pltpu.make_async_remote_copy(src_ref=src, dst_ref=dst, send_sem=send, recv_sem=recv, device_id=to, device_id_type=MESH)

    h_copy = remote(h_v.at[s], h_v.at[s], h_sem.at[0], h_sem.at[1], (dp, mate))

    def to_mate(j):
        return remote(pk_v.at[j, 1 - s], kv_v.at[j, mine], send_sem.at[0], kv_sem.at[j, mine], (dp, mate))

    def to_up(j, core):
        return remote(pk_v.at[j, core], kv_v.at[j, mine], send_sem.at[1], kv_sem.at[j, mine], dev(up, core))

    def to_down(j, core):
        return remote(pk_v.at[j, core], kv_v.at[j, mine], send_sem.at[2], kv_sem.at[j, mine], dev(down, core))

    def relay(j, block, chip):
        return remote(kv_v.at[j, block], kv_v.at[j, block], send_sem.at[3], kv_sem.at[j, block], dev(chip, s))

    def kv_wait(j, block):
        remote(kv_v.at[j, block], kv_v.at[j, block], send_sem.at[0], kv_sem.at[j, block], (dp, mate)).wait_recv()

    def o_copy(j, part=None):
        theirs = 1 - s
        if part is None:
            return remote(oo_v.at[j, theirs], or_v.at[j], o_sem.at[0], o_sem.at[1 + j], (dp, mate))
        return remote(oo_v.at[j, theirs, part], or_v.at[j, part], o_sem.at[0], o_sem.at[1 + j], (dp, mate))

    sends_down = jnp.logical_or(first, jnp.logical_and(c == 1, s == 1))
    second = c == 1
    even, odd = s == 0, s == 1
    third = c == 2

    def both(a, b):
        return jnp.logical_and(a, b)

    routes = ((0, 3, down), (1, 0, up), (2, 2, up), (3, 1, down))

    def relay_now(j, chips):
        for chip, block, to in routes[chips]:
            @pl.when(c == chip)
            def _():
                kv_wait(j, block)
                relay(j, block, to).start()

    loads[1].wait()
    for load in stages[2:]:
        load.start()
    loads[0].wait()
    wq_load(0).start()
    gain = jnp.concatenate([ln_v[k:k + 1, :] for k in range(feats // head)], axis=1).astype(F32)
    step = 64

    def norm_rows(r, _):
        x = x_v[0, pl.ds(pl.multiple_of(r * step, step), step), :].astype(F32)
        inv = lax.rsqrt(jnp.mean(x * x, axis=-1, keepdims=True) + EPS)
        h_v[s, pl.ds(pl.multiple_of(r * step, step), step), :] = (x * inv * gain).astype(BF16)
        return 0

    lax.fori_loop(0, rows // step, norm_rows, 0)
    wq_load(1).start()
    loads[5].start()
    pl.semaphore_wait(barrier, 1 + 2 * CORES)
    h_copy.start()
    for load in loads[2:5]:
        load.wait()
    k_gain = kg_v[...].astype(F32).reshape(1, head)

    def norm_rope(t, g, cos, sin):
        t = t * lax.rsqrt(jnp.mean(t * t, axis=-1, keepdims=True) + EPS) * g
        return (t * cos + pltpu.roll(t, head // 2, 1) * sin).astype(BF16)

    def finish_kv(j):
        for core in range(CORES):
            pk_v[j, core, 0] = norm_rope(raw_v[j, :rows, core * head:(core + 1) * head], k_gain, rope_v[0], rope_v[1])
            pk_v[j, core, 1] = raw_v[j, :rows, kvw + core * head:kvw + (core + 1) * head].T.astype(BF16)

    def send_up(j):
        for core in range(CORES):
            to_up(j, core).start()

    def send_down(j):
        for core in range(CORES):
            to_down(j, core).start()

    def send(when, *calls):
        @pl.when(when)
        def _():
            for call, j in calls:
                call(j)

    def send_kv(j):
        if j == 0:
            send(jnp.logical_or(third, both(c < 2, even)), (send_up, 0))
            send(both(c < 2, odd), (send_down, 0))
        else:
            send(both(first, even), (send_down, 0), (send_up, 1))
            send(both(second, odd), (send_up, 0), (send_down, 1))
            send(both(third, even), (send_up, 1))
        to_mate(j).start()
        kv_v[j, mine] = pk_v[j, s]

    def send_rest(part):
        if part == 0:
            send(both(first, odd), (send_up, 0), (send_up, 1), (send_down, 1))
            send(both(second, even), (send_up, 1))
        else:
            relay_now(0, slice(0, 4))
            send(both(first, even), (send_down, 1))
            send(jnp.logical_or(both(second, odd), both(third, odd)), (send_up, 1))

    for j in range(halves):
        pltpu.make_async_copy(wkv_v.at[j], wkv_v.at[j], wkv_sem.at[j]).wait()
        if j == 0:
            wq_load(2).start()
        raw_v[j, :rows, :2 * kvw] = jnp.dot(h_v[s], wkv_v[j], preferred_element_type=F32)
        finish_kv(j)
        send_kv(j)

    h_copy.wait_recv()

    def turn(t):
        return jnp.concatenate([t[head // 2:], t[:head // 2]], axis=0)

    def finish_q(i):
        for g in range(qcols // head):
            t = raw_v[i % 2, :, g * head:(g + 1) * head].T
            t = t * lax.rsqrt(jnp.mean(t * t, axis=0, keepdims=True) + EPS)
            q_v[i * (qcols // head) + g] = (t * ropet_v[0] + turn(t) * ropet_v[1]).astype(BF16)

    for i in range(2):
        wq_load(i).wait()
        cols = slice(i * halfq, (i + 1) * halfq)
        raw_v[0, :, cols] = jnp.dot(h_v[...].reshape(pair, feats), wq_v[0, :, cols], preferred_element_type=F32)
    send_rest(0)
    loads[5].wait()
    q_gain = jnp.broadcast_to(qg_v[...].astype(F32), (head, head)).T
    q_gain = jnp.concatenate([q_gain] * CORES, axis=1)

    ropet_v[0] = ropet_v[0] * q_gain
    ropet_v[1] = ropet_v[1] * turn(q_gain)

    for i in range(1, n_wq):
        wq_load(i + 1).wait()
        wo_load(s, wo_sem.at[0]).start()
        for n in (1 - s, CORES + s, CORES + 1 - s):
            wo_load(n, wo_sem.at[1]).start()
        raw_v[i] = jnp.dot(h_v[...].reshape(pair, feats), wq_v[i], preferred_element_type=F32)
        finish_q(i - 1)

    def attend(j, pieces, diagonal):
        keys = [kv_v[j, piece, 0] for piece in pieces]
        keys = [jnp.concatenate(keys[n:n + CORES], axis=0) for n in range(0, len(pieces), CORES)]
        vals = jnp.concatenate([kv_v[j, piece, 1] for piece in pieces], axis=1)
        span = len(pieces) * rows
        if diagonal:
            key = lax.broadcasted_iota(jnp.int32, (rows, rows), 0)
            row = lax.broadcasted_iota(jnp.int32, (rows, rows), 1)
            seen = key <= row

            def hide(sc):
                return jnp.where(seen, sc, -jnp.inf)

        def score(g):
            i = j * group + g
            top = None
            if diagonal:
                early = jnp.dot(keys[0][:rows], q_v[i], preferred_element_type=F32)
                early = jnp.concatenate([hide(early[:, :rows]), early[:, rows:]], axis=1)
                late = hide(jnp.dot(keys[0][rows:], q_v[i, :, rows:], preferred_element_type=F32))
                s_v[i, :rows] = early
                s_v[i, rows:pair, rows:] = late
                top = jnp.max(early, axis=0, keepdims=True)
                both = jnp.maximum(top[:, rows:], jnp.max(late, axis=0, keepdims=True))
                return jnp.concatenate([top[:, :rows], both], axis=1) * scale
            for n in range(len(keys)):
                sc = jnp.dot(keys[n], q_v[i], preferred_element_type=F32)
                s_v[i, n * pair:(n + 1) * pair] = sc
                best = jnp.max(sc, axis=0, keepdims=True) * scale
                top = best if top is None else jnp.maximum(top, best)
            return top

        def mix(g, new):
            i = j * group + g
            if not diagonal:
                old = m_v[i]
                new = jnp.maximum(old, new)
            m_v[i] = new
            if diagonal:
                early = jnp.exp2(s_v[i, :rows] * scale - new)
                late = jnp.exp2(s_v[i, rows:pair, rows:] * scale - new[:, rows:])
                total = jnp.sum(early, axis=0, keepdims=True)
                total = jnp.concatenate([total[:, :rows], total[:, rows:] + jnp.sum(late, axis=0, keepdims=True)], axis=1)
                probs = jnp.concatenate([early, jnp.concatenate([jnp.zeros_like(late), late], axis=1)], axis=0)
            else:
                probs = jnp.exp2(s_v[i, :span] * scale - new)
                total = jnp.sum(probs, axis=0, keepdims=True)
            mixed = jnp.dot(vals, probs.astype(BF16), preferred_element_type=F32)
            if diagonal:
                l_v[i] = total
                acc_v[i] = mixed
            else:
                fade = jnp.exp2(old - new)
                l_v[i] = l_v[i] * fade + total
                acc_v[i] = acc_v[i] * fade + mixed

        tops = [score(g) for g in range(group)]
        for g in range(group):
            mix(g, tops[g])

    def project(part, cols):
        o_ref, i = part
        return jnp.dot(jnp.concatenate([o_ref[0], o_ref[1]], axis=1), wo_v[i, :, cols], preferred_element_type=F32)

    for j in range(halves):
        kv_wait(j, mate)
    send_rest(1)
    finish_q(n_wq - 1)
    for j in range(halves):
        attend(j, [c * CORES, c * CORES + 1], True)

    relay_now(1, slice(0, 2))

    @pl.when(last)
    def _():
        for piece in (4, 5, 0):
            kv_wait(0, piece)
        attend(0, (4, 5, 0, 1), False)
        kv_wait(1, 1)
        relay(1, 1, down).start()

    def one_step(n, _):
        is3 = lax.div(c, 3)
        is2 = lax.div(c, 2) - is3
        half = lax.div(n, 2)
        odd_step = lax.rem(n, 2)
        even_step = 1 - odd_step
        j = half + is3 * lax.div(3 - n, 3)
        piece0 = is3 * (even_step * (4 + half) + odd_step * 2) + is2 * 2 * even_step
        piece1 = is3 * (even_step * (1 - half) + odd_step * 3) + is2 * (2 * even_step + 1) + (1 - is3 - is2)

        @pl.when(jnp.logical_or(both(third, n % 2 == 1), last))
        def _():
            kv_wait(j, piece0)

        @pl.when(jnp.logical_or(jnp.logical_or(both(second, n % 2 == 1), third), both(last, n > 0)))
        def _():
            kv_wait(j, piece1)

        @pl.when(jnp.logical_or(c > 1, both(second, n % 2 == 1)))
        def _():
            attend(j, (piece0, piece1), False)

        @pl.when(both(third, n == 0))
        def _():
            kv_wait(1, 2)
            relay(1, 2, up).start()

        def finish_o(j, heads):
            for g in heads:
                i = j * group + g
                o = acc_v[i] * (1.0 / l_v[i])
                part, at = divmod(g, group // 2)
                for core in range(CORES):
                    oo_v[j, core, part, :, at * head:(at + 1) * head] = o[:, core * rows:(core + 1) * rows].T.astype(BF16)

        @pl.when(n == 1)
        def _():
            finish_o(0, range(group))
            o_copy(0).start()

        @pl.when(n == 2 * halves - 1)
        def _():
            for part in range(2):
                finish_o(1, range(part * (group // 2), (part + 1) * (group // 2)))
                o_copy(1, part).start()

        @pl.when(n == 1)
        def _():
            wo_load(s, wo_sem.at[0]).wait()
            for k in range(feats // ocols):
                cols = slice(k * ocols, (k + 1) * ocols)
                y_v[:, cols] = x_v[0, :, cols].astype(F32) + project((oo_v.at[0, s], s), cols)

        return 0

    lax.fori_loop(0, 2 * halves, one_step, 0)
    pltpu.make_async_copy(wo_v.at[pl.ds(1, n_wo - 1)], wo_v.at[pl.ds(1, n_wo - 1)], wo_sem.at[1]).wait()
    o_copy(0).wait_recv()
    for k in range(feats // ocols):
        cols = slice(k * ocols, (k + 1) * ocols)
        y_v[:, cols] += project((or_v.at[0], 1 - s), cols) + project((oo_v.at[1, s], CORES + s), cols)
    o_copy(1).wait_recv()
    for k in range(feats // ocols):
        cols = slice(k * ocols, (k + 1) * ocols)
        out_v[:, cols] = (y_v[:, cols] + project((or_v.at[1], CORES + 1 - s), cols)).astype(BF16)

    h_copy.wait_send()
    theirs = 1 - s
    remote(pk_v.at[:, theirs], kv_v.at[:, mine], send_sem.at[0], kv_sem.at[0, 0], (dp, mate)).wait_send()
    remote(oo_v.at[:, theirs], or_v, o_sem.at[0], o_sem.at[1], (dp, mate)).wait_send()

    def sent(sem):
        remote(pk_v, kv_v.at[:, pl.ds(0, CORES)], sem, kv_sem.at[0, 0], (dp, mate)).wait_send()

    pl.when(jnp.logical_not(last))(functools.partial(sent, send_sem.at[1]))
    pl.when(sends_down)(functools.partial(sent, send_sem.at[2]))
    remote(kv_v.at[:, 0], kv_v.at[:, 0], send_sem.at[3], kv_sem.at[0, 0], (dp, mate)).wait_send()


def solution(mesh):
    group_size = mesh.shape['sp']
    assert group_size == CORES * CHIPS

    def device_step(hidden, ln_gain, w_q, w_k, w_v, w_o, q_gain, k_gain):
        rows, feats = hidden.shape
        head = q_gain.shape[0]
        kv_heads = w_k.shape[1] // head
        q_heads = w_q.shape[1] // head
        halves = kv_heads // CORES
        group = q_heads // kv_heads
        width = group * head
        pair = CORES * rows
        qcols = width
        n_wq = halves * width // qcols
        tables = np.stack(rope_tables(group_size * rows, head))
        by_device = tables.reshape(2, group_size, rows, head).transpose(1, 0, 2, 3)
        by_chip = tables.reshape(2, CHIPS, pair, head).transpose(1, 0, 3, 2)
        dma = pltpu.SemaphoreType.DMA
        any_spec = pl.BlockSpec(memory_space=pl.ANY)
        scratch = [
            pltpu.VMEM((1, rows, feats), BF16),
            pltpu.VMEM((feats // head, head), BF16),
            pltpu.VMEM((1, head), BF16),
            pltpu.VMEM((1, head), BF16),
            pltpu.VMEM((2, rows, head), F32),
            pltpu.VMEM((2, head, pair), F32),
            pltpu.VMEM((halves, feats, 2 * CORES * head), BF16),
            pltpu.VMEM((n_wq, feats, qcols), BF16),
            pltpu.VMEM((kv_heads, width, feats), BF16),
            pltpu.VMEM((CORES, rows, feats), BF16),
            pltpu.VMEM((halves, CORES, 2, rows, head), BF16),
            pltpu.VMEM((halves, group_size, 2, rows, head), BF16),
            pltpu.VMEM((2, pair, qcols), F32),
            pltpu.VMEM((halves * group, head, pair), BF16),
            pltpu.VMEM((halves * group, 2 * pair, pair), F32),
            pltpu.VMEM((halves * group, head, pair), F32),
            pltpu.VMEM((halves * group, 1, pair), F32),
            pltpu.VMEM((halves * group, 1, pair), F32),
            pltpu.VMEM((halves, CORES, 2, rows, width // 2), BF16),
            pltpu.VMEM((halves, 2, rows, width // 2), BF16),
            pltpu.VMEM((rows, feats), F32),
            dma((6,)), dma((halves,)), dma((n_wq + 1,)), dma((2,)), dma((2,)), dma((4,)), dma((halves, group_size)), dma((1 + halves,)),
        ]
        mixed = pl.pallas_call(
            kernel,
            out_shape=pltpu.VMEM((rows, feats), BF16),
            in_specs=[any_spec] * 10,
            out_specs=pl.BlockSpec(memory_space=pltpu.VMEM),
            scratch_shapes=scratch,
            compiler_params=pltpu.CompilerParams(
                collective_id=0, has_side_effects=True, vmem_limit_bytes=56 * 2 ** 20
            ),
            name="attention_block",
        )(hidden, ln_gain.reshape(-1, head), w_q, w_k, w_v, w_o, q_gain.reshape(1, -1), k_gain.reshape(1, -1),
          jnp.asarray(by_device), jnp.asarray(by_chip))
        return mixed

    row_spec = P(('dp', 'sp'), None)
    return jax.shard_map(device_step, mesh=mesh, in_specs=(row_spec, P(), P(), P(), P(), P(), P(), P()), out_specs=row_spec, check_vma=False)
```

```python
import functools
import numpy as np
import jax
import jax.numpy as jnp
from jax import lax
from jax.experimental import pallas as pl
from jax.experimental.pallas import tpu as pltpu
from jax.sharding import PartitionSpec as P

EPS = 1e-6
THETA = 1000000.0
LOG2E = 1.4426950408889634
MESH = pl.DeviceIdType.MESH
CORES = 2
CHIPS = 4
BF16 = jnp.bfloat16
F32 = jnp.float32


def rope_tables(rows, head_dim):
    half = head_dim // 2
    inv_freq = np.power(np.float32(THETA), -(np.arange(half, dtype=np.float32) * np.float32(2.0 / head_dim)))
    angles = np.arange(rows, dtype=np.float32)[:, None] * inv_freq.astype(np.float32)[None, :]
    cos = np.cos(angles.astype(np.float64)).astype(np.float32)
    sin = np.sin(angles.astype(np.float64)).astype(np.float32)
    return np.concatenate([cos, cos], axis=1), np.concatenate([-sin, sin], axis=1)


def kernel(x_hbm, ln_hbm, wq_hbm, wk_hbm, wv_hbm, wo_hbm, qg_hbm, kg_hbm, rope_hbm, ropet_hbm, out_v,
           x_v, ln_v, qg_v, kg_v, rope_v, ropet_v, wkv_v, wq_v, wo_v, h_v, pk_v, kv_v, raw_v, q_v, s_v, acc_v, m_v, l_v,
           oo_v, or_v, y_v,
           ld_sem, wkv_sem, h_sem, send_sem, kv_sem, o_sem):
    rows, feats = x_v.shape[1], x_v.shape[2]
    head = rope_v.shape[-1]
    pair = CORES * rows
    halves = wkv_v.shape[0]
    group = q_v.shape[0] // halves
    width = group * head
    scale = head ** -0.5 * LOG2E
    qcols = wq_v.shape[2]
    qparts = width // qcols
    ocols = 512

    dp = lax.axis_index("dp")
    sp = lax.axis_index("sp")
    c = lax.div(sp, CORES)
    s = lax.rem(sp, CORES)
    mate = c * CORES + (1 - s)
    up = lax.rem(c + 1, CHIPS)
    down = lax.rem(c + CHIPS - 1, CHIPS)
    first, last = c == 0, c == CHIPS - 1
    mine = c * CORES + s

    def dev(chip, core):
        return (dp, chip * CORES + core)

    loads = [
        pltpu.make_async_copy(x_hbm, x_v.at[0], ld_sem.at[0]),
        pltpu.make_async_copy(ln_hbm, ln_v, ld_sem.at[1]),
        pltpu.make_async_copy(qg_hbm, qg_v, ld_sem.at[2]),
        pltpu.make_async_copy(kg_hbm, kg_v, ld_sem.at[3]),
        pltpu.make_async_copy(rope_hbm.at[c * CORES + s], rope_v, ld_sem.at[4]),
        pltpu.make_async_copy(ropet_hbm.at[c], ropet_v, ld_sem.at[5]),
    ]
    kvw = CORES * head

    def wkv_load(j, which):
        src = (wk_hbm, wv_hbm)[which]
        return pltpu.make_async_copy(src.at[:, pl.ds(j * kvw, kvw)], wkv_v.at[j, :, pl.ds(which * kvw, kvw)], wkv_sem.at[j])

    halfq = qcols // 2

    def wq_load(i):
        if i < 2:
            col = s * width + i * halfq
            return pltpu.make_async_copy(wq_hbm.at[:, pl.ds(pl.multiple_of(col, halfq), halfq)], wq_v.at[0, :, pl.ds(i * halfq, halfq)], ld_sem.at[i])
        col = (CORES * (i - 1) + s) * width
        return pltpu.make_async_copy(wq_hbm.at[:, pl.ds(pl.multiple_of(col, qcols), qcols)], wq_v.at[i - 1], ld_sem.at[i])

    def wo_load(i, sem):
        return pltpu.make_async_copy(wo_hbm.at[pl.ds(pl.multiple_of(i * width, width), width)], wo_v.at[i], sem)

    n_wq = halves * qparts
    n_wo = CORES * halves
    stages = [wkv_load(j, which) for j in range(halves) for which in range(2)]
    for load in loads[:5] + stages[:2]:
        load.start()

    barrier = pltpu.get_barrier_semaphore()
    pl.semaphore_signal(barrier, inc=1, device_id=(dp, mate), device_id_type=MESH)
    for chip in (up, down):
        for core in range(CORES):
            pl.semaphore_signal(barrier, inc=1, device_id=dev(chip, core), device_id_type=MESH)

    def remote(src, dst, send, recv, to):
        return pltpu.make_async_remote_copy(src_ref=src, dst_ref=dst, send_sem=send, recv_sem=recv, device_id=to, device_id_type=MESH)

    h_copy = remote(h_v.at[s], h_v.at[s], h_sem.at[0], h_sem.at[1], (dp, mate))

    def to_mate(j):
        return remote(pk_v.at[j, 1 - s], kv_v.at[j, mine], send_sem.at[0], kv_sem.at[j, mine], (dp, mate))

    def to_up(j, core):
        return remote(pk_v.at[j, core], kv_v.at[j, mine], send_sem.at[1], kv_sem.at[j, mine], dev(up, core))

    def to_down(j, core):
        return remote(pk_v.at[j, core], kv_v.at[j, mine], send_sem.at[2], kv_sem.at[j, mine], dev(down, core))

    def relay(j, block, chip):
        return remote(kv_v.at[j, block], kv_v.at[j, block], send_sem.at[3], kv_sem.at[j, block], dev(chip, s))

    def kv_wait(j, block):
        remote(kv_v.at[j, block], kv_v.at[j, block], send_sem.at[0], kv_sem.at[j, block], (dp, mate)).wait_recv()

    def o_copy(j, part=None):
        theirs = 1 - s
        if part is None:
            return remote(oo_v.at[j, theirs], or_v.at[j], o_sem.at[0], o_sem.at[1 + j], (dp, mate))
        return remote(oo_v.at[j, theirs, part], or_v.at[j, part], o_sem.at[0], o_sem.at[1 + j], (dp, mate))

    sends_down = jnp.logical_or(first, jnp.logical_and(c == 1, s == 1))
    second = c == 1
    even, odd = s == 0, s == 1
    third = c == 2

    def both(a, b):
        return jnp.logical_and(a, b)

    routes = ((0, 3, down), (1, 0, up), (2, 2, up), (3, 1, down))

    def relay_now(j, chips):
        for chip, block, to in routes[chips]:
            @pl.when(c == chip)
            def _():
                kv_wait(j, block)
                relay(j, block, to).start()

    loads[1].wait()
    for load in stages[2:]:
        load.start()
    loads[0].wait()
    wq_load(0).start()
    gain = jnp.concatenate([ln_v[k:k + 1, :] for k in range(feats // head)], axis=1).astype(F32)
    step = 64

    def norm_rows(r, _):
        x = x_v[0, pl.ds(pl.multiple_of(r * step, step), step), :].astype(F32)
        inv = lax.rsqrt(jnp.mean(x * x, axis=-1, keepdims=True) + EPS)
        h_v[s, pl.ds(pl.multiple_of(r * step, step), step), :] = (x * inv * gain).astype(BF16)
        return 0

    lax.fori_loop(0, rows // step, norm_rows, 0)
    wq_load(1).start()
    loads[5].start()
    pl.semaphore_wait(barrier, 1 + 2 * CORES)
    h_copy.start()
    for load in loads[2:5]:
        load.wait()
    k_gain = kg_v[...].astype(F32).reshape(1, head)

    def norm_rope(t, g, cos, sin):
        t = t * lax.rsqrt(jnp.mean(t * t, axis=-1, keepdims=True) + EPS) * g
        return (t * cos + pltpu.roll(t, head // 2, 1) * sin).astype(BF16)

    def finish_kv(j):
        for core in range(CORES):
            pk_v[j, core, 0] = norm_rope(raw_v[j, :rows, core * head:(core + 1) * head], k_gain, rope_v[0], rope_v[1])
            pk_v[j, core, 1] = raw_v[j, :rows, kvw + core * head:kvw + (core + 1) * head].T.astype(BF16)

    def send_up(j):
        for core in range(CORES):
            to_up(j, core).start()

    def send_down(j):
        for core in range(CORES):
            to_down(j, core).start()

    def send(when, *calls):
        @pl.when(when)
        def _():
            for call, j in calls:
                call(j)

    def send_kv(j):
        if j == 0:
            send(jnp.logical_or(third, both(c < 2, even)), (send_up, 0))
            send(both(c < 2, odd), (send_down, 0))
        else:
            send(both(first, even), (send_down, 0), (send_up, 1))
            send(both(second, odd), (send_up, 0), (send_down, 1))
            send(both(third, even), (send_up, 1))
        to_mate(j).start()
        kv_v[j, mine] = pk_v[j, s]

    def send_rest(part):
        if part == 0:
            send(both(first, odd), (send_up, 0), (send_up, 1), (send_down, 1))
            send(both(second, even), (send_up, 1))
        else:
            relay_now(0, slice(0, 4))
            send(both(first, even), (send_down, 1))
            send(jnp.logical_or(both(second, odd), both(third, odd)), (send_up, 1))

    for j in range(halves):
        pltpu.make_async_copy(wkv_v.at[j], wkv_v.at[j], wkv_sem.at[j]).wait()
        if j == 0:
            wq_load(2).start()
        raw_v[j, :rows, :2 * kvw] = jnp.dot(h_v[s], wkv_v[j], preferred_element_type=F32)
        finish_kv(j)
        send_kv(j)

    h_copy.wait_recv()

    def turn(t):
        return jnp.concatenate([t[head // 2:], t[:head // 2]], axis=0)

    def finish_q(i):
        for g in range(qcols // head):
            t = raw_v[i % 2, :, g * head:(g + 1) * head].T
            t = t * lax.rsqrt(jnp.mean(t * t, axis=0, keepdims=True) + EPS)
            q_v[i * (qcols // head) + g] = (t * ropet_v[0] + turn(t) * ropet_v[1]).astype(BF16)

    for i in range(2):
        wq_load(i).wait()
        cols = slice(i * halfq, (i + 1) * halfq)
        raw_v[0, :, cols] = jnp.dot(h_v[...].reshape(pair, feats), wq_v[0, :, cols], preferred_element_type=F32)
    send_rest(0)
    loads[5].wait()
    q_gain = jnp.broadcast_to(qg_v[...].astype(F32), (head, head)).T
    q_gain = jnp.concatenate([q_gain] * CORES, axis=1)

    ropet_v[0] = ropet_v[0] * q_gain
    ropet_v[1] = ropet_v[1] * turn(q_gain)

    for i in range(1, n_wq):
        wq_load(i + 1).wait()
        wo_load(s, wkv_sem.at[0]).start()
        for n in (1 - s, CORES + s, CORES + 1 - s):
            wo_load(n, wkv_sem.at[1]).start()
        raw_v[i] = jnp.dot(h_v[...].reshape(pair, feats), wq_v[i], preferred_element_type=F32)
        finish_q(i - 1)

    def attend(j, pieces, diagonal):
        keys = [kv_v[j, piece, 0] for piece in pieces]
        keys = [jnp.concatenate(keys[n:n + CORES], axis=0) for n in range(0, len(pieces), CORES)]
        vals = jnp.concatenate([kv_v[j, piece, 1] for piece in pieces], axis=1)
        span = len(pieces) * rows
        if diagonal:
            key = lax.broadcasted_iota(jnp.int32, (rows, rows), 0)
            row = lax.broadcasted_iota(jnp.int32, (rows, rows), 1)
            seen = key <= row

            def hide(sc):
                return jnp.where(seen, sc, -jnp.inf)

        def score(g):
            i = j * group + g
            top = None
            if diagonal:
                early = jnp.dot(keys[0][:rows], q_v[i], preferred_element_type=F32)
                early = jnp.concatenate([hide(early[:, :rows]), early[:, rows:]], axis=1)
                late = hide(jnp.dot(keys[0][rows:], q_v[i, :, rows:], preferred_element_type=F32))
                s_v[i, :rows] = early
                s_v[i, rows:pair, rows:] = late
                top = jnp.max(early, axis=0, keepdims=True)
                both = jnp.maximum(top[:, rows:], jnp.max(late, axis=0, keepdims=True))
                return jnp.concatenate([top[:, :rows], both], axis=1) * scale
            for n in range(len(keys)):
                sc = jnp.dot(keys[n], q_v[i], preferred_element_type=F32)
                s_v[i, n * pair:(n + 1) * pair] = sc
                best = jnp.max(sc, axis=0, keepdims=True) * scale
                top = best if top is None else jnp.maximum(top, best)
            return top

        def mix(g, new):
            i = j * group + g
            if not diagonal:
                old = m_v[i]
                new = jnp.maximum(old, new)
            m_v[i] = new
            if diagonal:
                early = jnp.exp2(s_v[i, :rows] * scale - new)
                late = jnp.exp2(s_v[i, rows:pair, rows:] * scale - new[:, rows:])
                total = jnp.sum(early, axis=0, keepdims=True)
                total = jnp.concatenate([total[:, :rows], total[:, rows:] + jnp.sum(late, axis=0, keepdims=True)], axis=1)
                probs = jnp.concatenate([early, jnp.concatenate([jnp.zeros_like(late), late], axis=1)], axis=0)
            else:
                probs = jnp.exp2(s_v[i, :span] * scale - new)
                total = jnp.sum(probs, axis=0, keepdims=True)
            mixed = jnp.dot(vals, probs.astype(BF16), preferred_element_type=F32)
            if diagonal:
                l_v[i] = total
                acc_v[i] = mixed
            else:
                fade = jnp.exp2(old - new)
                l_v[i] = l_v[i] * fade + total
                acc_v[i] = acc_v[i] * fade + mixed

        tops = [score(g) for g in range(group)]
        for g in range(group):
            mix(g, tops[g])

    def project(part, cols):
        o_ref, i = part
        return jnp.dot(jnp.concatenate([o_ref[0], o_ref[1]], axis=1), wo_v[i, :, cols], preferred_element_type=F32)

    for j in range(halves):
        kv_wait(j, mate)
    send_rest(1)
    finish_q(n_wq - 1)
    for j in range(halves):
        attend(j, [c * CORES, c * CORES + 1], True)

    relay_now(1, slice(0, 2))

    @pl.when(last)
    def _():
        for piece in (4, 5, 0):
            kv_wait(0, piece)
        attend(0, (4, 5, 0, 1), False)
        kv_wait(1, 1)
        relay(1, 1, down).start()

    def one_step(n, _):
        is3 = lax.div(c, 3)
        is2 = lax.div(c, 2) - is3
        half = lax.div(n, 2)
        odd_step = lax.rem(n, 2)
        even_step = 1 - odd_step
        j = half + is3 * lax.div(3 - n, 3)
        piece0 = is3 * (even_step * (4 + half) + odd_step * 2) + is2 * 2 * even_step
        piece1 = is3 * (even_step * (1 - half) + odd_step * 3) + is2 * (2 * even_step + 1) + (1 - is3 - is2)

        @pl.when(jnp.logical_or(both(third, n % 2 == 1), last))
        def _():
            kv_wait(j, piece0)

        @pl.when(jnp.logical_or(jnp.logical_or(both(second, n % 2 == 1), third), both(last, n > 0)))
        def _():
            kv_wait(j, piece1)

        @pl.when(jnp.logical_or(c > 1, both(second, n % 2 == 1)))
        def _():
            attend(j, (piece0, piece1), False)

        @pl.when(both(third, n == 0))
        def _():
            kv_wait(1, 2)
            relay(1, 2, up).start()

        def finish_o(j, heads):
            for g in heads:
                i = j * group + g
                o = acc_v[i] * (1.0 / l_v[i])
                part, at = divmod(g, group // 2)
                for core in range(CORES):
                    oo_v[j, core, part, :, at * head:(at + 1) * head] = o[:, core * rows:(core + 1) * rows].T.astype(BF16)

        @pl.when(n == 1)
        def _():
            finish_o(0, range(group))
            o_copy(0).start()

        @pl.when(n == 2 * halves - 1)
        def _():
            for part in range(2):
                finish_o(1, range(part * (group // 2), (part + 1) * (group // 2)))
                o_copy(1, part).start()

        @pl.when(n == 1)
        def _():
            wo_load(s, wkv_sem.at[0]).wait()
            for k in range(feats // ocols):
                cols = slice(k * ocols, (k + 1) * ocols)
                y_v[:, cols] = x_v[0, :, cols].astype(F32) + project((oo_v.at[0, s], s), cols)

        return 0

    lax.fori_loop(0, 2 * halves, one_step, 0)
    pltpu.make_async_copy(wo_v.at[pl.ds(1, n_wo - 1)], wo_v.at[pl.ds(1, n_wo - 1)], wkv_sem.at[1]).wait()
    o_copy(0).wait_recv()
    for k in range(feats // ocols):
        cols = slice(k * ocols, (k + 1) * ocols)
        y_v[:, cols] += project((or_v.at[0], 1 - s), cols) + project((oo_v.at[1, s], CORES + s), cols)
    o_copy(1).wait_recv()
    for k in range(feats // ocols):
        cols = slice(k * ocols, (k + 1) * ocols)
        out_v[:, cols] = (y_v[:, cols] + project((or_v.at[1], CORES + 1 - s), cols)).astype(BF16)

    h_copy.wait_send()
    theirs = 1 - s
    remote(pk_v.at[:, theirs], kv_v.at[:, mine], send_sem.at[0], kv_sem.at[0, 0], (dp, mate)).wait_send()
    remote(oo_v.at[:, theirs], or_v, o_sem.at[0], o_sem.at[1], (dp, mate)).wait_send()

    def sent(sem):
        remote(pk_v, kv_v.at[:, pl.ds(0, CORES)], sem, kv_sem.at[0, 0], (dp, mate)).wait_send()

    pl.when(jnp.logical_not(last))(functools.partial(sent, send_sem.at[1]))
    pl.when(sends_down)(functools.partial(sent, send_sem.at[2]))
    remote(kv_v.at[:, 0], kv_v.at[:, 0], send_sem.at[3], kv_sem.at[0, 0], (dp, mate)).wait_send()


def solution(mesh):
    group_size = mesh.shape['sp']
    assert group_size == CORES * CHIPS

    def device_step(hidden, ln_gain, w_q, w_k, w_v, w_o, q_gain, k_gain):
        rows, feats = hidden.shape
        head = q_gain.shape[0]
        kv_heads = w_k.shape[1] // head
        q_heads = w_q.shape[1] // head
        halves = kv_heads // CORES
        group = q_heads // kv_heads
        width = group * head
        pair = CORES * rows
        qcols = width
        n_wq = halves * width // qcols
        tables = np.stack(rope_tables(group_size * rows, head))
        by_device = tables.reshape(2, group_size, rows, head).transpose(1, 0, 2, 3)
        by_chip = tables.reshape(2, CHIPS, pair, head).transpose(1, 0, 3, 2)
        dma = pltpu.SemaphoreType.DMA
        any_spec = pl.BlockSpec(memory_space=pl.ANY)
        scratch = [
            pltpu.VMEM((1, rows, feats), BF16),
            pltpu.VMEM((feats // head, head), BF16),
            pltpu.VMEM((1, head), BF16),
            pltpu.VMEM((1, head), BF16),
            pltpu.VMEM((2, rows, head), F32),
            pltpu.VMEM((2, head, pair), F32),
            pltpu.VMEM((halves, feats, 2 * CORES * head), BF16),
            pltpu.VMEM((n_wq, feats, qcols), BF16),
            pltpu.VMEM((kv_heads, width, feats), BF16),
            pltpu.VMEM((CORES, rows, feats), BF16),
            pltpu.VMEM((halves, CORES, 2, rows, head), BF16),
            pltpu.VMEM((halves, group_size, 2, rows, head), BF16),
            pltpu.VMEM((2, pair, qcols), F32),
            pltpu.VMEM((halves * group, head, pair), BF16),
            pltpu.VMEM((halves * group, 2 * pair, pair), F32),
            pltpu.VMEM((halves * group, head, pair), F32),
            pltpu.VMEM((halves * group, 1, pair), F32),
            pltpu.VMEM((halves * group, 1, pair), F32),
            pltpu.VMEM((halves, CORES, 2, rows, width // 2), BF16),
            pltpu.VMEM((halves, 2, rows, width // 2), BF16),
            pltpu.VMEM((rows, feats), F32),
            dma((6,)), dma((halves,)), dma((2,)), dma((4,)), dma((halves, group_size)), dma((1 + halves,)),
        ]
        mixed = pl.pallas_call(
            kernel,
            out_shape=pltpu.VMEM((rows, feats), BF16),
            in_specs=[any_spec] * 10,
            out_specs=pl.BlockSpec(memory_space=pltpu.VMEM),
            scratch_shapes=scratch,
            compiler_params=pltpu.CompilerParams(
                collective_id=0, has_side_effects=True, vmem_limit_bytes=56 * 2 ** 20
            ),
            name="attention_block",
        )(hidden, ln_gain.reshape(-1, head), w_q, w_k, w_v, w_o, q_gain.reshape(1, -1), k_gain.reshape(1, -1),
          jnp.asarray(by_device), jnp.asarray(by_chip))
        return mixed

    row_spec = P(('dp', 'sp'), None)
    return jax.shard_map(device_step, mesh=mesh, in_specs=(row_spec, P(), P(), P(), P(), P(), P(), P()), out_specs=row_spec, check_vma=False)
```
